128 devices in a mesh: tm: 16 (over y_hi, z, core), bank: 8 (over y_lo, x).
Axes of the slice: x: 4, y: 4 (y_hi: 2, y_lo: 2; y = y_hi * 2 + y_lo), z: 4, core: 2. Of those that a mesh axis runs over, the one named last changes fastest.
Arguments:
- strain: float32 [32, 131072], P('tm', 'bank'), may hold values from -40 to 40
- lengths: int32 [32], P('tm'), may hold values from 65536 to 131072
- templates: bfloat16 [2, 32, 512, 512], P(None, 'bank'), may hold values from -6 to 6
Outputs:
- snr: float32 [32, 4194304], P('bank', 'tm')
The draws below stay inside these ranges and needn't reach their ends.
All inputs are finite; a program needn't handle non-finite values.
Results may differ from the reference program's by a relative error of at most 0.014.
Values may be sent and summed in bfloat16 or wider, within the bound.
A program may use at most 128 MiB of HBM per device.

```python
import math
import jax
import jax.numpy as jnp
from jax import lax

R = 512
BLOCK = 131072
BLOCKS = 32
NTEMP = 32


line_count = 64


def draw_strain(key, part):
    noise_key, freq_key, phase_key, amp_key = jax.random.split(jax.random.fold_in(key, 7), 4)
    position = jnp.arange(BLOCKS * BLOCK, dtype=jnp.float32).reshape(BLOCKS, BLOCK)
    fraction = position / (BLOCKS * BLOCK)
    noise = jax.random.truncated_normal(noise_key, -6.0, 6.0, (BLOCKS, BLOCK), jnp.float32)
    envelope = 1.0 + 2.0 * fraction
    freqs = jax.random.uniform(freq_key, (line_count,), jnp.float32, 0.01, 0.49)
    phases = jax.random.uniform(phase_key, (line_count,), jnp.float32, 0.0, 2.0 * math.pi)
    amplitudes = jnp.exp(jax.random.uniform(amp_key, (line_count,), jnp.float32, math.log(0.01), math.log(0.3)))

    def add_line(total, item):
        frequency, phase, amplitude = item
        cycles = jnp.mod(frequency * position, 1.0)
        return (total + amplitude * jnp.cos(2.0 * math.pi * cycles + phase), None)
    lines, unused = lax.scan(add_line, jnp.zeros((BLOCKS, BLOCK), jnp.float32), (freqs, phases, amplitudes))
    return noise * envelope + lines


def touch_ends(array, own_key, smallest, largest):
    longest = array.shape.index(max(array.shape))
    spots = []
    for shift in (0, 1):
        where = [jax.random.randint(jax.random.fold_in(own_key, axis), (), 0, length) for axis, length in enumerate(array.shape)]
        where[longest] = (where[longest] + shift) % array.shape[longest]
        spots.append(tuple(where))
    return array.at[spots[0]].set(smallest).at[spots[1]].set(largest)


def shard_levels(rng, extent, shards, low, top_value):
    loudness = 1.0
    for dim, blocks in shards:
        steps = jax.random.uniform(jax.random.fold_in(jax.random.fold_in(rng, 6), dim), (blocks,), jnp.float32, low / len(shards), top_value / len(shards))
        loudness = loudness * jnp.repeat(jnp.exp(steps), extent[dim] // blocks).reshape((-1,) + (1,) * (len(extent) - 1 - dim))
    return loudness


def gaussian(own_key, extent, spread, most, shards=(), kind=jnp.bfloat16):
    array = jax.random.normal(own_key, extent, jnp.float32) * spread
    if len(shards) > 0:
        array = shard_levels(own_key, extent, shards, -0.22, 0.18) * array
    return jnp.clip(array, min=-most, max=most).astype(kind)


def setup_inputs(seed: int = 0) -> dict:
    key_of = jax.random.split(jax.random.key(seed), 4)
    strain = draw_strain(jax.random.fold_in(key_of[3], 71), 0)
    lengths = touch_ends(jax.random.randint(key_of[1], (BLOCKS,), BLOCK // 2, BLOCK + 1), jax.random.fold_in(key_of[1], 1), BLOCK // 2, BLOCK).astype(jnp.int32)
    templates = gaussian(key_of[2], (2, NTEMP, R, R), 1.0, 6.0, ((1, 8),))
    return {"strain": strain, "lengths": lengths, "templates": templates}


epsilon = 1e-06
two_pi = 2.0 * math.pi

def dft_tables(order):
    index = jnp.arange(order, dtype=jnp.int32)
    product = index[:, None] * index[None, :]
    angle = (product % order).astype(jnp.float32) * (two_pi / order)
    twist = product.astype(jnp.float32) * (two_pi / (order * order))
    return (jnp.cos(angle).astype(jnp.bfloat16), jnp.sin(angle).astype(jnp.bfloat16), jnp.cos(twist), jnp.sin(twist))

def rounded(values):
    return lax.optimization_barrier(values.astype(jnp.bfloat16)).astype(jnp.float32)

def reference(strain, lengths, templates):
    cosine, sine, twist_cos, twist_sin = dft_tables(R)
    cos_full = cosine.astype(jnp.float32)
    sin_full = sine.astype(jnp.float32)
    half_rows = R // 2
    position = jnp.arange(BLOCK, dtype=jnp.int32)
    valid = position[None, :] < lengths[:, None]
    gated = rounded(jnp.where(valid, strain, 0.0)).reshape(BLOCKS, half_rows, R)
    first_real = jnp.einsum('kn,cnm->ckm', cos_full[:, :half_rows], gated)
    first_imag = -jnp.einsum('kn,cnm->ckm', sin_full[:, :half_rows], gated)
    twist_real = rounded(first_real * twist_cos + first_imag * twist_sin)
    twist_imag = rounded(first_imag * twist_cos - first_real * twist_sin)
    spec_real = jnp.einsum('ckn,nm->ckm', twist_real, cos_full) + jnp.einsum('ckn,nm->ckm', twist_imag, sin_full)
    spec_imag = jnp.einsum('ckn,nm->ckm', twist_imag, cos_full) - jnp.einsum('ckn,nm->ckm', twist_real, sin_full)
    power = lax.optimization_barrier(jnp.sum(spec_real * spec_real + spec_imag * spec_imag, axis=0))
    weight = lax.rsqrt(power / BLOCKS + epsilon)
    white_real = rounded(spec_real * weight)
    white_imag = rounded(spec_imag * weight)

    def filter_one(template_pair):
        tmpl_real = template_pair[0].astype(jnp.float32)
        tmpl_imag = template_pair[1].astype(jnp.float32)
        prod_real = rounded(tmpl_real * white_real + tmpl_imag * white_imag)
        prod_imag = rounded(tmpl_real * white_imag - tmpl_imag * white_real)
        inner_real = jnp.einsum('ckm,mn->ckn', prod_real, cos_full) - jnp.einsum('ckm,mn->ckn', prod_imag, sin_full)
        inner_imag = jnp.einsum('ckm,mn->ckn', prod_real, sin_full) + jnp.einsum('ckm,mn->ckn', prod_imag, cos_full)
        back_real = rounded(inner_real * twist_cos - inner_imag * twist_sin)
        back_imag = rounded(inner_imag * twist_cos + inner_real * twist_sin)
        output = jnp.einsum('nk,ckm->cnm', cos_full, back_real) - jnp.einsum('nk,ckm->cnm', sin_full, back_imag)
        factor = lax.rsqrt(jnp.sum(tmpl_real * tmpl_real + tmpl_imag * tmpl_imag))
        flat = output.reshape(BLOCKS, R * R)
        own_part = flat[:, :BLOCK] * factor
        tail_part = flat[:, BLOCK:] * factor
        previous = jnp.concatenate([jnp.zeros((1, BLOCK), own_part.dtype), tail_part[:-1]], axis=0)
        return (own_part + previous).reshape(BLOCKS * BLOCK)
    moved = jnp.moveaxis(templates, 1, 0)
    return lax.map(filter_one, moved)
```

```python
import functools
import math

import jax
import jax.numpy as jnp
import numpy as np
from jax import lax
from jax.experimental import pallas as pl
from jax.experimental.pallas import tpu as pltpu
from jax.sharding import PartitionSpec as P

R = 512
HALF = 256
ROWS = 272
RADIX = 4
Q = 128
epsilon = 1e-06
MESH = pl.DeviceIdType.MESH


def tables():
    k = np.arange(HALF + 1, dtype=np.int64)
    u = np.arange(R, dtype=np.int64)
    angle = 2.0 * math.pi * ((k[:, None] * u[None, :]) % R) / R
    first = np.zeros((2 * ROWS, R), np.float64)
    first[: HALF + 1] = np.cos(angle)
    first[ROWS : ROWS + HALF + 1] = -np.sin(angle)
    turn = 2.0 * math.pi * (k[:, None] * u[None, :]) / (R * R)
    tc = np.zeros((ROWS, R), np.float64)
    ts = np.zeros((ROWS, R), np.float64)
    tc[: HALF + 1] = np.cos(turn)
    ts[: HALF + 1] = np.sin(turn)
    v = np.arange(Q, dtype=np.int64)
    fwd = np.zeros((RADIX, HALF, HALF), np.float64)
    inv = np.zeros((RADIX, HALF, HALF), np.float64)
    for r in range(RADIX):
        phase = 2.0 * math.pi * ((v[:, None] * (RADIX * v[None, :] + r)) % R) / R
        c, s = np.cos(phase), np.sin(phase)
        fwd[r] = np.block([[c, -s], [s, c]])
        inv[r] = np.block([[c.T, s.T], [-s.T, c.T]])
    w = np.arange(HALF, dtype=np.int64)
    last = np.zeros((HALF, R), np.float64)
    phase = 2.0 * math.pi * ((w[:, None] * k[None, :HALF]) % R) / R
    last[:, :HALF] = np.cos(phase)
    last[:, HALF:] = -np.sin(phase)
    last[:, HALF] = 1.0 - 2.0 * (w % 2)
    return first, tc, ts, fwd, inv, last


def half(x):
    return x.astype(jnp.bfloat16)


def full(x):
    return x.astype(jnp.float32)


def dot(a, b):
    return jnp.dot(a, b, preferred_element_type=jnp.float32)


CHUNKS = ((0, 128), (128, 144))


def inverse_kernel(z_ref, g_ref, fac_ref, inv_ref, tc_ref, ts_ref, last_ref, out_ref, back, y, sem):
    j = pl.program_id(0)
    slot = lax.rem(j, 2)

    def copies(at, which):
        return [
            pltpu.make_async_copy(
                y.at[which, q, :, pl.ds(m * Q, Q)],
                out_ref.at[pl.ds(q * HALF, HALF), m, at, :],
                sem.at[which, q * RADIX + m],
            )
            for q in range(2)
            for m in range(RADIX)
        ]

    @pl.when(j >= 2)
    def _():
        for c in copies(j - 2, slot):
            c.wait()

    factor = fac_ref[0, 0:1, 0:1]
    for q in range(2):
        for start, size in CHUNKS:
            rows = pl.ds(start, size)
            tr, ti = [], []
            for r in range(RADIX):
                lo = r * 2 * Q
                zr = full(z_ref[q, rows, lo : lo + Q])
                zi = full(z_ref[q, rows, lo + Q : lo + 2 * Q])
                gr = full(g_ref[0, rows, lo : lo + Q])
                gi = full(g_ref[0, rows, lo + Q : lo + 2 * Q])
                prod = jnp.concatenate([half(gr * zr + gi * zi), half(gr * zi - gi * zr)], axis=1)
                t = dot(prod, inv_ref[r])
                tr.append(t[:, :Q])
                ti.append(t[:, Q:])
            ar, ai, br, bi = tr[0] + tr[2], ti[0] + ti[2], tr[0] - tr[2], ti[0] - ti[2]
            cr, ci, dr, di = tr[1] + tr[3], ti[1] + ti[3], tr[1] - tr[3], ti[1] - ti[3]
            inner = ((ar + cr, ai + ci), (br - di, bi + dr), (ar - cr, ai - ci), (br + di, bi - dr))
            for m in range(RADIX):
                lanes = slice(m * Q, (m + 1) * Q)
                ir, ii = inner[m]
                tc, ts = tc_ref[rows, lanes], ts_ref[rows, lanes]
                real = half(ir * tc - ii * ts)
                imag = half(ii * tc + ir * ts)
                keep = min(size, HALF - start)
                back[q, pl.ds(start, keep), lanes] = real[:keep]
                if start == 0:
                    back[q, pl.ds(HALF, keep), lanes] = imag[:keep]
                else:
                    back[q, pl.ds(HALF + start, keep), lanes] = imag[:keep]
                    top = back[q, HALF : HALF + 16, lanes]
                    first_row = lax.broadcasted_iota(jnp.int32, (16, Q), 0) == 0
                    back[q, HALF : HALF + 16, lanes] = half(
                        jnp.where(first_row, full(real[keep : keep + 16]), full(top))
                    )
        y[slot, q] = dot(last_ref[...], back[q]) * factor

    for c in copies(j, slot):
        c.start()

    @pl.when(j == pl.num_programs(0) - 1)
    def _():
        for c in copies(j - 1, 1 - slot):
            c.wait()
        for c in copies(j, slot):
            c.wait()


def inverse(z, g, fac, inv, tc, ts, last):
    n = g.shape[0]
    whole = lambda *shape: pl.BlockSpec(shape, lambda j: (0,) * len(shape))
    return pl.pallas_call(
        inverse_kernel,
        grid=(n,),
        in_specs=[
            whole(2, ROWS, 2 * R),
            pl.BlockSpec((1, ROWS, 2 * R), lambda j: (j, 0, 0)),
            pl.BlockSpec((1, 8, Q), lambda j: (j, 0, 0)),
            whole(RADIX, HALF, HALF),
            whole(ROWS, R),
            whole(ROWS, R),
            whole(HALF, R),
        ],
        out_specs=pl.BlockSpec(memory_space=pl.ANY),
        out_shape=jax.ShapeDtypeStruct((2 * HALF, RADIX, n, Q), jnp.float32),
        scratch_shapes=[
            pltpu.VMEM((2, R, R), jnp.bfloat16),
            pltpu.VMEM((2, 2, HALF, R), jnp.float32),
            pltpu.SemaphoreType.DMA((2, 2 * RADIX)),
        ],
        compiler_params=pltpu.CompilerParams(vmem_limit_bytes=32 << 20),
        name="inverse",
    )(z, g, fac, inv, tc, ts, last)


def fill_slot(i, lanes):
    return slice(i * lanes, (i + 1) * lanes)


def forward(fr, fi, tc, ts, fwd_ref):
    tr = fr * tc + fi * ts
    ti = fi * tc - fr * ts
    r0, r1, r2, r3 = (tr[:, fill_slot(m, Q)] for m in range(RADIX))
    i0, i1, i2, i3 = (ti[:, fill_slot(m, Q)] for m in range(RADIX))
    ar, ai, br, bi = r0 + r2, i0 + i2, r0 - r2, i0 - i2
    cr, ci, dr, di = r1 + r3, i1 + i3, r1 - r3, i1 - i3
    parts = ((ar + cr, ai + ci), (br + di, bi - dr), (ar - cr, ai - ci), (br - di, bi + dr))
    return [
        dot(jnp.concatenate([half(x), half(y)], axis=1), fwd_ref[r])
        for r, (x, y) in enumerate(parts)
    ]


def spectrum_kernel(
    tm, bank, total_blocks,
    strain_ref, lens_ref, tmpl_hbm, first_hbm, tc_hbm, ts_hbm, fwd_hbm,
    z_ref, g_ref, fac_ref,
    raw, blocks, prev, tmpl, first, tc, ts, fwd, zraw, send, recv, weights,
    load_sem, gather_send, gather_recv, sum_send, sum_recv, prev_send, prev_recv,
    share_send, share_recv,
):
    t = lax.axis_index("tm")
    b = lax.axis_index("bank")
    piece = HALF // bank
    band = HALF // bank
    tiles = band // 8 * RADIX

    loads = []
    for c in range(2):
        for m in range(RADIX):
            loads.append((strain_ref.at[:, m, c, :], raw.at[c, :, pl.ds(m * Q, Q)]))
    loads += [(first_hbm, first), (tc_hbm, tc), (ts_hbm, ts), (fwd_hbm, fwd), (tmpl_hbm, tmpl)]
    loads = [pltpu.make_async_copy(s, d, load_sem.at[i]) for i, (s, d) in enumerate(loads)]
    for load in loads:
        load.start()

    barrier = pltpu.get_barrier_semaphore()
    for i in range(1, bank):
        pl.semaphore_signal(
            barrier, 1, device_id={"tm": t, "bank": lax.rem(b + i, bank)}, device_id_type=MESH
        )
    for i in range(1, tm):
        pl.semaphore_signal(
            barrier, 1, device_id={"tm": lax.rem(t + i, tm), "bank": b}, device_id_type=MESH
        )

    for load in loads[: 2 * RADIX]:
        load.wait()
    own_rows = pl.ds(pl.multiple_of(b * piece, piece), piece)
    position = (
        (lax.broadcasted_iota(jnp.int32, (piece, R), 0) + b * piece) * R
        + lax.broadcasted_iota(jnp.int32, (piece, R), 1)
    )
    for c in range(2):
        blocks[c, own_rows, :] = half(jnp.where(position < lens_ref[c], raw[c], 0.0))

    @pl.when(t == 0)
    def _():
        prev[...] = jnp.zeros_like(prev)

    pl.semaphore_wait(barrier, bank + tm - 2)

    def gather_copy(i):
        return pltpu.make_async_remote_copy(
            src_ref=blocks.at[:, own_rows, :],
            dst_ref=blocks.at[:, own_rows, :],
            send_sem=gather_send.at[i],
            recv_sem=gather_recv.at[i],
            device_id={"tm": t, "bank": lax.rem(b + i, bank)},
            device_id_type=MESH,
        )

    def gather_arrival(i):
        source = lax.rem(b - i + bank, bank)
        rows = pl.ds(pl.multiple_of(source * piece, piece), piece)
        return pltpu.make_async_remote_copy(
            src_ref=blocks.at[:, rows, :],
            dst_ref=blocks.at[:, rows, :],
            send_sem=gather_send.at[i],
            recv_sem=gather_recv.at[i],
            device_id={"tm": t, "bank": source},
            device_id_type=MESH,
        )

    for i in range(1, bank):
        gather_copy(i).start()

    for load in loads[2 * RADIX :]:
        load.wait()
    row = lax.broadcasted_iota(jnp.int32, (R, R), 0)
    col = lax.broadcasted_iota(jnp.int32, (R, R), 1)
    order = lax.rem(col, Q) * RADIX + lax.div(col, Q)
    pick = half(jnp.where(row == order, 1.0, 0.0))
    pick_mirror = half(jnp.where(row == R - 1 - order, 1.0, 0.0))
    up = lax.broadcasted_iota(jnp.int32, (ROWS, HALF), 0)
    across = lax.broadcasted_iota(jnp.int32, (ROWS, HALF), 1)
    flip = half(jnp.where(jnp.logical_and(across == HALF - up, across > 0), 1.0, 0.0))

    def join(j, carry):
        norm = jnp.zeros((1, R), jnp.float32)
        for p in range(2):
            direct = dot(tmpl[p, j, 0:ROWS, :], pick)
            mirror = dot(flip, half(dot(tmpl[p, j, HALF:R, :], pick_mirror)))
            joined = half(direct + mirror if p == 0 else direct - mirror)
            for r in range(RADIX):
                lo = (2 * r + p) * Q
                g_ref[j, :, lo : lo + Q] = joined[:, fill_slot(r, Q)]
            values = full(tmpl[p, j])
            norm = norm + jnp.sum(values * values, axis=0, keepdims=True)
        factor = lax.rsqrt(jnp.sum(norm, axis=1, keepdims=True))
        fac_ref[j] = jnp.broadcast_to(factor, (8, Q))
        return carry

    lax.fori_loop(0, g_ref.shape[0], join, 0)

    for i in range(1, bank):
        gather_arrival(i).wait_recv()

    low = pl.ds(pl.multiple_of(b * band, band), band)
    low_imag = pl.ds(pl.multiple_of(ROWS + b * band, 16), band)
    table = jnp.concatenate(
        [
            first[low, 0:HALF],
            first[HALF:ROWS, 0:HALF],
            first[low_imag, 0:HALF],
            first[ROWS + HALF : 2 * ROWS, 0:HALF],
        ],
        axis=0,
    )
    band_tc = jnp.concatenate([tc[low, :], tc[HALF:ROWS, :]], axis=0)
    band_ts = jnp.concatenate([ts[low, :], ts[HALF:ROWS, :]], axis=0)
    power = [0.0] * RADIX
    height = band + ROWS - HALF
    for c in range(2):
        f = dot(table, blocks[c])
        spec = forward(f[:height], f[height:], band_tc, band_ts, fwd)
        for r in range(RADIX):
            re, im = spec[r][:, :Q], spec[r][:, Q:]
            power[r] = power[r] + (re * re + im * im)
    extra = jnp.concatenate(
        [power[r][band : band + 1] for r in range(RADIX)] + [jnp.zeros((8 - RADIX, Q), jnp.float32)],
        axis=0,
    )
    for i in range(tiles):
        at = i // RADIX * 8
        send[i, 0:8, :] = power[i % RADIX][at : at + 8]
        send[i, 8:16, :] = extra

    def sum_copy(i):
        to = lax.rem(t + i, tm)
        return pltpu.make_async_remote_copy(
            src_ref=send.at[to],
            dst_ref=recv.at[t],
            send_sem=sum_send.at[i],
            recv_sem=sum_recv.at[i],
            device_id={"tm": to, "bank": b},
            device_id_type=MESH,
        )

    def sum_arrival(i):
        source = lax.rem(t - i + tm, tm)
        return pltpu.make_async_remote_copy(
            src_ref=send.at[source],
            dst_ref=recv.at[source],
            send_sem=sum_send.at[i],
            recv_sem=sum_recv.at[i],
            device_id={"tm": source, "bank": b},
            device_id_type=MESH,
        )

    for i in range(1, tm):
        sum_copy(i).start()
    recv[t] = send[t]

    next_copy = pltpu.make_async_remote_copy(
        src_ref=blocks.at[1],
        dst_ref=prev,
        send_sem=prev_send,
        recv_sem=prev_recv,
        device_id={"tm": lax.rem(t + 1, tm), "bank": b},
        device_id_type=MESH,
    )

    @pl.when(t < tm - 1)
    def _():
        next_copy.start()

    def region(q, now, before):
        f = dot(first[:, 0:HALF], now) + dot(first[:, HALF:R], before)
        spec = forward(f[:ROWS], f[ROWS:], tc[...], ts[...], fwd)
        for r in range(RADIX):
            zraw[q, :, fill_slot(r, 2 * Q)] = spec[r]

    region(1, blocks[1], blocks[0])

    for i in range(1, tm):
        sum_arrival(i).wait_recv()
    total = recv[0]
    for i in range(1, tm):
        total = total + recv[i]
    weight = lax.rsqrt(total * (1.0 / total_blocks) + epsilon)
    me = b * tm + t
    weights[me] = half(weight[0:8])

    def share_copy(to_t, to_b, slot):
        return pltpu.make_async_remote_copy(
            src_ref=weights.at[slot],
            dst_ref=weights.at[slot],
            send_sem=share_send,
            recv_sem=share_recv,
            device_id={"tm": to_t, "bank": to_b},
            device_id_type=MESH,
        )

    def share(i, carry):
        share_copy(lax.rem(t + lax.div(i, bank), tm), lax.rem(b + lax.rem(i, bank), bank), me).start()
        return carry

    lax.fori_loop(1, tm * bank, share, 0)

    @pl.when(t > 0)
    def _():
        next_copy.wait_recv()

    region(0, blocks[0], prev[...])

    others = pltpu.make_async_remote_copy(
        src_ref=weights.at[pl.ds(0, tm * bank - 1)],
        dst_ref=weights.at[pl.ds(0, tm * bank - 1)],
        send_sem=share_send,
        recv_sem=share_recv,
        device_id={"tm": t, "bank": lax.rem(b + 1, bank)},
        device_id_type=MESH,
    )
    others.wait_recv()

    def whiten(i, carry):
        rows = pl.ds(pl.multiple_of(i * 16, 16), 16)
        for r in range(RADIX):
            at = 2 * i * RADIX + r
            w = jnp.concatenate([full(weights[at]), full(weights[at + RADIX])], axis=0)
            for q in range(2):
                for p in range(2):
                    lanes = fill_slot(2 * r + p, Q)
                    z_ref[q, rows, lanes] = half(zraw[q, rows, lanes] * w)
        return carry

    lax.fori_loop(0, HALF // 16, whiten, 0)
    for r in range(RADIX):
        for q in range(2):
            for p in range(2):
                lanes = fill_slot(2 * r + p, Q)
                z_ref[q, HALF:ROWS, lanes] = half(
                    zraw[q, HALF:ROWS, lanes] * weight[8 + r : 9 + r]
                )

    for i in range(1, bank):
        gather_copy(i).wait_send()
    for i in range(1, tm):
        sum_copy(i).wait_send()

    @pl.when(t < tm - 1)
    def _():
        next_copy.wait_send()

    others.wait_send()


def spectra(strain, lengths, templates, tabs, tm, bank):
    n = templates.shape[1]
    first, tc, ts, fwd = tabs
    anyspace = pl.BlockSpec(memory_space=pl.ANY)
    vmem = pl.BlockSpec(memory_space=pltpu.VMEM)
    bf, f32 = jnp.bfloat16, jnp.float32
    sem = pltpu.SemaphoreType.DMA
    pieces = strain.reshape(2, HALF // bank * RADIX, Q).transpose(1, 0, 2)
    pieces = pieces.reshape(HALF // bank, RADIX, 2, Q)
    return pl.pallas_call(
        functools.partial(spectrum_kernel, tm, bank, 2 * tm),
        in_specs=[anyspace, pl.BlockSpec(memory_space=pltpu.SMEM)] + [anyspace] * 5,
        out_specs=[vmem] * 3,
        out_shape=[
            jax.ShapeDtypeStruct((2, ROWS, 2 * R), bf),
            jax.ShapeDtypeStruct((n, ROWS, 2 * R), bf),
            jax.ShapeDtypeStruct((n, 8, Q), f32),
        ],
        scratch_shapes=[
            pltpu.VMEM((2, HALF // bank, R), f32),
            pltpu.VMEM((2, HALF, R), bf),
            pltpu.VMEM((HALF, R), bf),
            pltpu.VMEM((2, n, R, R), bf),
            pltpu.VMEM((2 * ROWS, R), bf),
            pltpu.VMEM((ROWS, R), f32),
            pltpu.VMEM((ROWS, R), f32),
            pltpu.VMEM((RADIX, HALF, HALF), bf),
            pltpu.VMEM((2, ROWS, 2 * R), f32),
            pltpu.VMEM((tm, 16, Q), f32),
            pltpu.VMEM((tm, 16, Q), f32),
            pltpu.VMEM((tm * bank, 8, Q), bf),
            sem((2 * RADIX + 5,)),
            sem((bank,)),
            sem((bank,)),
            sem((tm,)),
            sem((tm,)),
            sem,
            sem,
            sem,
            sem,
        ],
        compiler_params=pltpu.CompilerParams(
            collective_id=0, has_side_effects=True, vmem_limit_bytes=32 << 20
        ),
        name="spectra",
    )(pieces, lengths, templates, first, tc, ts, fwd)


def body(tm, bank, strain, lengths, templates):
    first, tc, ts, fwd, inv, last = tables()
    bf = lambda x: jnp.asarray(x, jnp.bfloat16)
    f32 = lambda x: jnp.asarray(x, jnp.float32)
    tc, ts = f32(tc), f32(ts)
    z, g, fac = spectra(strain, lengths, templates, (bf(first), tc, ts, bf(fwd)), tm, bank)
    out = inverse(z, g, fac, bf(inv), tc, ts, bf(last))
    n = templates.shape[1]
    return out.reshape(2 * HALF * RADIX, n, Q).transpose(1, 0, 2).reshape(n, 2 * HALF * R)


def solution(mesh):
    in_specs = (P("tm", "bank"), P("tm"), P(None, "bank", None, None))
    step = functools.partial(body, mesh.shape["tm"], mesh.shape["bank"])
    return jax.shard_map(
        step, mesh=mesh, in_specs=in_specs, out_specs=P("bank", "tm"), check_vma=False
    )
```

```python
import functools
import math

import jax
import jax.numpy as jnp
import numpy as np
from jax import lax
from jax.experimental import pallas as pl
from jax.experimental.pallas import tpu as pltpu
from jax.sharding import PartitionSpec as P

R = 512
HALF = 256
ROWS = 272
RADIX = 4
Q = 128
epsilon = 1e-06
MESH = pl.DeviceIdType.MESH


def tables():
    k = np.arange(HALF + 1, dtype=np.int64)
    u = np.arange(R, dtype=np.int64)
    angle = 2.0 * math.pi * ((k[:, None] * u[None, :]) % R) / R
    first = np.zeros((2 * ROWS, R), np.float64)
    first[: HALF + 1] = np.cos(angle)
    first[ROWS : ROWS + HALF + 1] = -np.sin(angle)
    turn = 2.0 * math.pi * (k[:, None] * u[None, :]) / (R * R)
    tc = np.zeros((ROWS, R), np.float64)
    ts = np.zeros((ROWS, R), np.float64)
    tc[: HALF + 1] = np.cos(turn)
    ts[: HALF + 1] = np.sin(turn)
    v = np.arange(Q, dtype=np.int64)
    fwd = np.zeros((RADIX, HALF, HALF), np.float64)
    inv = np.zeros((RADIX, HALF, HALF), np.float64)
    for r in range(RADIX):
        phase = 2.0 * math.pi * ((v[:, None] * (RADIX * v[None, :] + r)) % R) / R
        c, s = np.cos(phase), np.sin(phase)
        fwd[r] = np.block([[c, -s], [s, c]])
        inv[r] = np.block([[c.T, s.T], [-s.T, c.T]])
    w = np.arange(HALF, dtype=np.int64)
    last = np.zeros((HALF, R), np.float64)
    phase = 2.0 * math.pi * ((w[:, None] * k[None, :HALF]) % R) / R
    last[:, :HALF] = np.cos(phase)
    last[:, HALF:] = -np.sin(phase)
    last[:, HALF] = 1.0 - 2.0 * (w % 2)
    return first, tc, ts, fwd, inv, last


def half(x):
    return x.astype(jnp.bfloat16)


def full(x):
    return x.astype(jnp.float32)


def dot(a, b):
    return jnp.dot(a, b, preferred_element_type=jnp.float32)


CHUNKS = ((0, 128), (128, 144))


def inverse_kernel(z_ref, g_ref, fac_ref, inv_ref, tc_ref, ts_ref, last_ref, out_ref, back, y, sem):
    j = pl.program_id(0)
    slot = lax.rem(j, 2)

    def copies(at, which):
        return [
            pltpu.make_async_copy(
                y.at[which, q, :, pl.ds(m * Q, Q)],
                out_ref.at[pl.ds(q * HALF, HALF), m, at, :],
                sem.at[which, q * RADIX + m],
            )
            for q in range(2)
            for m in range(RADIX)
        ]

    @pl.when(j >= 2)
    def _():
        for c in copies(j - 2, slot):
            c.wait()

    factor = fac_ref[0, 0:1, 0:1]
    for q in range(2):
        for start, size in CHUNKS:
            rows = pl.ds(start, size)
            tr, ti = [], []
            for r in range(RADIX):
                lo = r * 2 * Q
                zr = full(z_ref[q, rows, lo : lo + Q])
                zi = full(z_ref[q, rows, lo + Q : lo + 2 * Q])
                gr = full(g_ref[0, rows, lo : lo + Q])
                gi = full(g_ref[0, rows, lo + Q : lo + 2 * Q])
                prod = jnp.concatenate([half(gr * zr + gi * zi), half(gr * zi - gi * zr)], axis=1)
                t = dot(prod, inv_ref[r])
                tr.append(t[:, :Q])
                ti.append(t[:, Q:])
            ar, ai, br, bi = tr[0] + tr[2], ti[0] + ti[2], tr[0] - tr[2], ti[0] - ti[2]
            cr, ci, dr, di = tr[1] + tr[3], ti[1] + ti[3], tr[1] - tr[3], ti[1] - ti[3]
            inner = ((ar + cr, ai + ci), (br - di, bi + dr), (ar - cr, ai - ci), (br + di, bi - dr))
            for m in range(RADIX):
                lanes = slice(m * Q, (m + 1) * Q)
                ir, ii = inner[m]
                tc, ts = tc_ref[rows, lanes], ts_ref[rows, lanes]
                real = half(ir * tc - ii * ts)
                imag = half(ii * tc + ir * ts)
                keep = min(size, HALF - start)
                back[q, pl.ds(start, keep), lanes] = real[:keep]
                if start == 0:
                    back[q, pl.ds(HALF, keep), lanes] = imag[:keep]
                else:
                    back[q, pl.ds(HALF + start, keep), lanes] = imag[:keep]
                    top = back[q, HALF : HALF + 16, lanes]
                    first_row = lax.broadcasted_iota(jnp.int32, (16, Q), 0) == 0
                    back[q, HALF : HALF + 16, lanes] = half(
                        jnp.where(first_row, full(real[keep : keep + 16]), full(top))
                    )
        y[slot, q] = dot(last_ref[...], back[q]) * factor

    for c in copies(j, slot):
        c.start()

    @pl.when(j == pl.num_programs(0) - 1)
    def _():
        for c in copies(j - 1, 1 - slot):
            c.wait()
        for c in copies(j, slot):
            c.wait()


def inverse(z, g, fac, inv, tc, ts, last):
    n = g.shape[0]
    whole = lambda *shape: pl.BlockSpec(shape, lambda j: (0,) * len(shape))
    return pl.pallas_call(
        inverse_kernel,
        grid=(n,),
        in_specs=[
            whole(2, ROWS, 2 * R),
            pl.BlockSpec((1, ROWS, 2 * R), lambda j: (j, 0, 0)),
            pl.BlockSpec((1, 8, Q), lambda j: (j, 0, 0)),
            whole(RADIX, HALF, HALF),
            whole(ROWS, R),
            whole(ROWS, R),
            whole(HALF, R),
        ],
        out_specs=pl.BlockSpec(memory_space=pl.ANY),
        out_shape=jax.ShapeDtypeStruct((2 * HALF, RADIX, n, Q), jnp.float32),
        scratch_shapes=[
            pltpu.VMEM((2, R, R), jnp.bfloat16),
            pltpu.VMEM((2, 2, HALF, R), jnp.float32),
            pltpu.SemaphoreType.DMA((2, 2 * RADIX)),
        ],
        compiler_params=pltpu.CompilerParams(vmem_limit_bytes=32 << 20),
        name="inverse",
    )(z, g, fac, inv, tc, ts, last)


def fill_slot(i, lanes):
    return slice(i * lanes, (i + 1) * lanes)


def forward(fr, fi, tc, ts, fwd_ref):
    tr = fr * tc + fi * ts
    ti = fi * tc - fr * ts
    r0, r1, r2, r3 = (tr[:, fill_slot(m, Q)] for m in range(RADIX))
    i0, i1, i2, i3 = (ti[:, fill_slot(m, Q)] for m in range(RADIX))
    ar, ai, br, bi = r0 + r2, i0 + i2, r0 - r2, i0 - i2
    cr, ci, dr, di = r1 + r3, i1 + i3, r1 - r3, i1 - i3
    parts = ((ar + cr, ai + ci), (br + di, bi - dr), (ar - cr, ai - ci), (br - di, bi + dr))
    return [
        dot(jnp.concatenate([half(x), half(y)], axis=1), fwd_ref[r])
        for r, (x, y) in enumerate(parts)
    ]


def spectrum_kernel(
    tm, bank, total_blocks,
    strain_ref, lens_hbm, tmpl_hbm, first_hbm, tc_hbm, ts_hbm, fwd_hbm,
    z_ref, g_ref, fac_ref,
    lens_ref, raw, blocks, prev, tmpl, first, tc, ts, fwd, zraw, send, recv, weights,
    load_sem, gather_send, gather_recv, sum_send, sum_recv, prev_send, prev_recv,
    share_send, share_recv,
):
    t = lax.axis_index("tm")
    b = lax.axis_index("bank")
    piece = HALF // bank
    band = HALF // bank
    tiles = band // 8 * RADIX

    loads = [(lens_hbm, lens_ref)]
    for c in range(2):
        for m in range(RADIX):
            loads.append((strain_ref.at[:, m, c, :], raw.at[c, :, pl.ds(m * Q, Q)]))
    loads += [(first_hbm, first), (tc_hbm, tc), (ts_hbm, ts), (fwd_hbm, fwd), (tmpl_hbm, tmpl)]
    loads = [pltpu.make_async_copy(s, d, load_sem.at[i]) for i, (s, d) in enumerate(loads)]
    for load in loads:
        load.start()

    barrier = pltpu.get_barrier_semaphore()
    for i in range(1, bank):
        pl.semaphore_signal(
            barrier, 1, device_id={"tm": t, "bank": lax.rem(b + i, bank)}, device_id_type=MESH
        )
    for i in range(1, tm):
        pl.semaphore_signal(
            barrier, 1, device_id={"tm": lax.rem(t + i, tm), "bank": b}, device_id_type=MESH
        )

    for load in loads[: 2 * RADIX + 1]:
        load.wait()
    own_rows = pl.ds(pl.multiple_of(b * piece, piece), piece)
    position = (
        (lax.broadcasted_iota(jnp.int32, (piece, R), 0) + b * piece) * R
        + lax.broadcasted_iota(jnp.int32, (piece, R), 1)
    )
    for c in range(2):
        blocks[c, own_rows, :] = half(jnp.where(position < lens_ref[c], raw[c], 0.0))

    @pl.when(t == 0)
    def _():
        prev[...] = jnp.zeros_like(prev)

    pl.semaphore_wait(barrier, bank + tm - 2)

    def gather_copy(i):
        return pltpu.make_async_remote_copy(
            src_ref=blocks.at[:, own_rows, :],
            dst_ref=blocks.at[:, own_rows, :],
            send_sem=gather_send.at[i],
            recv_sem=gather_recv.at[i],
            device_id={"tm": t, "bank": lax.rem(b + i, bank)},
            device_id_type=MESH,
        )

    def gather_arrival(i):
        source = lax.rem(b - i + bank, bank)
        rows = pl.ds(pl.multiple_of(source * piece, piece), piece)
        return pltpu.make_async_remote_copy(
            src_ref=blocks.at[:, rows, :],
            dst_ref=blocks.at[:, rows, :],
            send_sem=gather_send.at[i],
            recv_sem=gather_recv.at[i],
            device_id={"tm": t, "bank": source},
            device_id_type=MESH,
        )

    for i in range(1, bank):
        gather_copy(i).start()

    for load in loads[2 * RADIX + 1 :]:
        load.wait()
    row = lax.broadcasted_iota(jnp.int32, (R, R), 0)
    col = lax.broadcasted_iota(jnp.int32, (R, R), 1)
    order = lax.rem(col, Q) * RADIX + lax.div(col, Q)
    pick = half(jnp.where(row == order, 1.0, 0.0))
    pick_mirror = half(jnp.where(row == R - 1 - order, 1.0, 0.0))
    up = lax.broadcasted_iota(jnp.int32, (ROWS, HALF), 0)
    across = lax.broadcasted_iota(jnp.int32, (ROWS, HALF), 1)
    flip = half(jnp.where(jnp.logical_and(across == HALF - up, across > 0), 1.0, 0.0))

    def join(j, carry):
        norm = jnp.zeros((1, R), jnp.float32)
        for p in range(2):
            direct = dot(tmpl[p, j, 0:ROWS, :], pick)
            mirror = dot(flip, half(dot(tmpl[p, j, HALF:R, :], pick_mirror)))
            joined = half(direct + mirror if p == 0 else direct - mirror)
            for r in range(RADIX):
                lo = (2 * r + p) * Q
                g_ref[j, :, lo : lo + Q] = joined[:, fill_slot(r, Q)]
            values = full(tmpl[p, j])
            norm = norm + jnp.sum(values * values, axis=0, keepdims=True)
        factor = lax.rsqrt(jnp.sum(norm, axis=1, keepdims=True))
        fac_ref[j] = jnp.broadcast_to(factor, (8, Q))
        return carry

    lax.fori_loop(0, g_ref.shape[0], join, 0)

    for i in range(1, bank):
        gather_arrival(i).wait_recv()

    low = pl.ds(pl.multiple_of(b * band, band), band)
    low_imag = pl.ds(pl.multiple_of(ROWS + b * band, 16), band)
    table = jnp.concatenate(
        [
            first[low, 0:HALF],
            first[HALF:ROWS, 0:HALF],
            first[low_imag, 0:HALF],
            first[ROWS + HALF : 2 * ROWS, 0:HALF],
        ],
        axis=0,
    )
    band_tc = jnp.concatenate([tc[low, :], tc[HALF:ROWS, :]], axis=0)
    band_ts = jnp.concatenate([ts[low, :], ts[HALF:ROWS, :]], axis=0)
    power = [0.0] * RADIX
    height = band + ROWS - HALF
    for c in range(2):
        f = dot(table, blocks[c])
        spec = forward(f[:height], f[height:], band_tc, band_ts, fwd)
        for r in range(RADIX):
            re, im = spec[r][:, :Q], spec[r][:, Q:]
            power[r] = power[r] + (re * re + im * im)
    extra = jnp.concatenate(
        [power[r][band : band + 1] for r in range(RADIX)] + [jnp.zeros((8 - RADIX, Q), jnp.float32)],
        axis=0,
    )
    for i in range(tiles):
        at = i // RADIX * 8
        send[i, 0:8, :] = power[i % RADIX][at : at + 8]
        send[i, 8:16, :] = extra

    def sum_copy(i):
        to = lax.rem(t + i, tm)
        return pltpu.make_async_remote_copy(
            src_ref=send.at[to],
            dst_ref=recv.at[t],
            send_sem=sum_send.at[i],
            recv_sem=sum_recv.at[i],
            device_id={"tm": to, "bank": b},
            device_id_type=MESH,
        )

    def sum_arrival(i):
        source = lax.rem(t - i + tm, tm)
        return pltpu.make_async_remote_copy(
            src_ref=send.at[source],
            dst_ref=recv.at[source],
            send_sem=sum_send.at[i],
            recv_sem=sum_recv.at[i],
            device_id={"tm": source, "bank": b},
            device_id_type=MESH,
        )

    for i in range(1, tm):
        sum_copy(i).start()
    recv[t] = send[t]

    next_copy = pltpu.make_async_remote_copy(
        src_ref=blocks.at[1],
        dst_ref=prev,
        send_sem=prev_send,
        recv_sem=prev_recv,
        device_id={"tm": lax.rem(t + 1, tm), "bank": b},
        device_id_type=MESH,
    )

    @pl.when(t < tm - 1)
    def _():
        next_copy.start()

    def region(q, now, before):
        f = dot(first[:, 0:HALF], now) + dot(first[:, HALF:R], before)
        spec = forward(f[:ROWS], f[ROWS:], tc[...], ts[...], fwd)
        for r in range(RADIX):
            zraw[q, :, fill_slot(r, 2 * Q)] = spec[r]

    region(1, blocks[1], blocks[0])

    for i in range(1, tm):
        sum_arrival(i).wait_recv()
    total = recv[0]
    for i in range(1, tm):
        total = total + recv[i]
    weight = lax.rsqrt(total * (1.0 / total_blocks) + epsilon)
    me = b * tm + t
    weights[me] = half(weight[0:8])

    def share_copy(to_t, to_b, slot):
        return pltpu.make_async_remote_copy(
            src_ref=weights.at[slot],
            dst_ref=weights.at[slot],
            send_sem=share_send,
            recv_sem=share_recv,
            device_id={"tm": to_t, "bank": to_b},
            device_id_type=MESH,
        )

    def share(i, carry):
        share_copy(lax.rem(t + lax.div(i, bank), tm), lax.rem(b + lax.rem(i, bank), bank), me).start()
        return carry

    lax.fori_loop(1, tm * bank, share, 0)

    @pl.when(t > 0)
    def _():
        next_copy.wait_recv()

    region(0, blocks[0], prev[...])

    others = pltpu.make_async_remote_copy(
        src_ref=weights.at[pl.ds(0, tm * bank - 1)],
        dst_ref=weights.at[pl.ds(0, tm * bank - 1)],
        send_sem=share_send,
        recv_sem=share_recv,
        device_id={"tm": t, "bank": lax.rem(b + 1, bank)},
        device_id_type=MESH,
    )
    others.wait_recv()

    def whiten(i, carry):
        rows = pl.ds(pl.multiple_of(i * 16, 16), 16)
        for r in range(RADIX):
            at = 2 * i * RADIX + r
            w = jnp.concatenate([full(weights[at]), full(weights[at + RADIX])], axis=0)
            for q in range(2):
                for p in range(2):
                    lanes = fill_slot(2 * r + p, Q)
                    z_ref[q, rows, lanes] = half(zraw[q, rows, lanes] * w)
        return carry

    lax.fori_loop(0, HALF // 16, whiten, 0)
    for r in range(RADIX):
        for q in range(2):
            for p in range(2):
                lanes = fill_slot(2 * r + p, Q)
                z_ref[q, HALF:ROWS, lanes] = half(
                    zraw[q, HALF:ROWS, lanes] * weight[8 + r : 9 + r]
                )

    for i in range(1, bank):
        gather_copy(i).wait_send()
    for i in range(1, tm):
        sum_copy(i).wait_send()

    @pl.when(t < tm - 1)
    def _():
        next_copy.wait_send()

    others.wait_send()


def spectra(strain, lengths, templates, tabs, tm, bank):
    n = templates.shape[1]
    first, tc, ts, fwd = tabs
    hbm = pl.BlockSpec(memory_space=pltpu.HBM)
    vmem = pl.BlockSpec(memory_space=pltpu.VMEM)
    bf, f32 = jnp.bfloat16, jnp.float32
    sem = pltpu.SemaphoreType.DMA
    pieces = strain.reshape(2, HALF // bank * RADIX, Q).transpose(1, 0, 2)
    pieces = pieces.reshape(HALF // bank, RADIX, 2, Q)
    return pl.pallas_call(
        functools.partial(spectrum_kernel, tm, bank, 2 * tm),
        in_specs=[hbm] * 7,
        out_specs=[vmem] * 3,
        out_shape=[
            jax.ShapeDtypeStruct((2, ROWS, 2 * R), bf),
            jax.ShapeDtypeStruct((n, ROWS, 2 * R), bf),
            jax.ShapeDtypeStruct((n, 8, Q), f32),
        ],
        scratch_shapes=[
            pltpu.SMEM((2,), jnp.int32),
            pltpu.VMEM((2, HALF // bank, R), f32),
            pltpu.VMEM((2, HALF, R), bf),
            pltpu.VMEM((HALF, R), bf),
            pltpu.VMEM((2, n, R, R), bf),
            pltpu.VMEM((2 * ROWS, R), bf),
            pltpu.VMEM((ROWS, R), f32),
            pltpu.VMEM((ROWS, R), f32),
            pltpu.VMEM((RADIX, HALF, HALF), bf),
            pltpu.VMEM((2, ROWS, 2 * R), f32),
            pltpu.VMEM((tm, 16, Q), f32),
            pltpu.VMEM((tm, 16, Q), f32),
            pltpu.VMEM((tm * bank, 8, Q), bf),
            sem((2 * RADIX + 6,)),
            sem((bank,)),
            sem((bank,)),
            sem((tm,)),
            sem((tm,)),
            sem,
            sem,
            sem,
            sem,
        ],
        compiler_params=pltpu.CompilerParams(
            collective_id=0, has_side_effects=True, vmem_limit_bytes=32 << 20
        ),
        name="spectra",
    )(*[pltpu.with_memory_space_constraint(x, pltpu.HBM) for x in (pieces, lengths, templates, first, tc, ts, fwd)])


def body(tm, bank, strain, lengths, templates):
    first, tc, ts, fwd, inv, last = tables()
    bf = lambda x: jnp.asarray(x, jnp.bfloat16)
    f32 = lambda x: jnp.asarray(x, jnp.float32)
    tc, ts = f32(tc), f32(ts)
    z, g, fac = spectra(strain, lengths, templates, (bf(first), tc, ts, bf(fwd)), tm, bank)
    out = inverse(z, g, fac, bf(inv), tc, ts, bf(last))
    n = templates.shape[1]
    return out.reshape(2 * HALF * RADIX, n, Q).transpose(1, 0, 2).reshape(n, 2 * HALF * R)


def solution(mesh):
    in_specs = (P("tm", "bank"), P("tm"), P(None, "bank", None, None))
    step = functools.partial(body, mesh.shape["tm"], mesh.shape["bank"])
    return jax.shard_map(
        step, mesh=mesh, in_specs=in_specs, out_specs=P("bank", "tm"), check_vma=False
    )
```

```python
import functools
import math

import jax
import jax.numpy as jnp
import numpy as np
from jax import lax
from jax.experimental import pallas as pl
from jax.experimental.pallas import tpu as pltpu
from jax.sharding import PartitionSpec as P

R = 512
HALF = 256
ROWS = 272
RADIX = 4
Q = 128
epsilon = 1e-06
MESH = pl.DeviceIdType.MESH


def tables():
    k = np.arange(HALF + 1, dtype=np.int64)
    u = np.arange(R, dtype=np.int64)
    angle = 2.0 * math.pi * ((k[:, None] * u[None, :]) % R) / R
    first = np.zeros((2 * ROWS, R), np.float64)
    first[: HALF + 1] = np.cos(angle)
    first[ROWS : ROWS + HALF + 1] = -np.sin(angle)
    turn = 2.0 * math.pi * (k[:, None] * u[None, :]) / (R * R)
    tc = np.zeros((ROWS, R), np.float64)
    ts = np.zeros((ROWS, R), np.float64)
    tc[: HALF + 1] = np.cos(turn)
    ts[: HALF + 1] = np.sin(turn)
    v = np.arange(Q, dtype=np.int64)
    fwd = np.zeros((RADIX, HALF, HALF), np.float64)
    inv = np.zeros((RADIX, HALF, HALF), np.float64)
    for r in range(RADIX):
        phase = 2.0 * math.pi * ((v[:, None] * (RADIX * v[None, :] + r)) % R) / R
        c, s = np.cos(phase), np.sin(phase)
        fwd[r] = np.block([[c, -s], [s, c]])
        inv[r] = np.block([[c.T, s.T], [-s.T, c.T]])
    w = np.arange(HALF, dtype=np.int64)
    last = np.zeros((HALF, R), np.float64)
    phase = 2.0 * math.pi * ((w[:, None] * k[None, :HALF]) % R) / R
    last[:, :HALF] = np.cos(phase)
    last[:, HALF:] = -np.sin(phase)
    last[:, HALF] = 1.0 - 2.0 * (w % 2)
    return first, tc, ts, fwd, inv, last


def half(x):
    return x.astype(jnp.bfloat16)


def full(x):
    return x.astype(jnp.float32)


def dot(a, b):
    return jnp.dot(a, b, preferred_element_type=jnp.float32)


CHUNKS = ((0, 128), (128, 144))


def inner_rows(z_ref, g_ref, inv_ref, tc_ref, ts_ref, back, j, q, start, size):
    rows = pl.ds(start, size)
    tr, ti = [], []
    for r in range(RADIX):
        lo = r * 2 * Q
        zr = full(z_ref[q, rows, lo : lo + Q])
        zi = full(z_ref[q, rows, lo + Q : lo + 2 * Q])
        gr = full(g_ref[j, rows, lo : lo + Q])
        gi = full(g_ref[j, rows, lo + Q : lo + 2 * Q])
        prod = jnp.concatenate([half(gr * zr + gi * zi), half(gr * zi - gi * zr)], axis=1)
        t = dot(prod, inv_ref[r])
        tr.append(t[:, :Q])
        ti.append(t[:, Q:])
    ar, ai, br, bi = tr[0] + tr[2], ti[0] + ti[2], tr[0] - tr[2], ti[0] - ti[2]
    cr, ci, dr, di = tr[1] + tr[3], ti[1] + ti[3], tr[1] - tr[3], ti[1] - ti[3]
    inner = ((ar + cr, ai + ci), (br - di, bi + dr), (ar - cr, ai - ci), (br + di, bi - dr))
    for m in range(RADIX):
        lanes = slice(m * Q, (m + 1) * Q)
        ir, ii = inner[m]
        tc, ts = tc_ref[rows, lanes], ts_ref[rows, lanes]
        real = half(ir * tc - ii * ts)
        imag = half(ii * tc + ir * ts)
        keep = min(size, HALF - start)
        back[pl.ds(start, keep), lanes] = real[:keep]
        back[pl.ds(HALF + start, keep), lanes] = imag[:keep]
        if start + size == ROWS:
            top = back[HALF : HALF + 16, lanes]
            first_row = lax.broadcasted_iota(jnp.int32, (16, Q), 0) == 0
            back[HALF : HALF + 16, lanes] = half(
                jnp.where(first_row, full(real[keep : keep + 16]), full(top))
            )


def inverse_kernel(n, z_ref, g_ref, fac_ref, inv_ref, tc_ref, ts_ref, last_ref, out_ref, back, y, sem):
    copies = []

    def last_rows(j, q):
        y[j, q] = dot(last_ref[...], back[j % 2, q]) * fac_ref[j, 0:1, 0:1]
        for m in range(RADIX):
            copy = pltpu.make_async_copy(
                y.at[j, q, :, pl.ds(m * Q, Q)],
                out_ref.at[pl.ds(q * HALF, HALF), m, j, :],
                sem.at[j, q * RADIX + m],
            )
            copy.start()
            copies.append(copy)

    steps = [(j, q) for j in range(n) for q in range(2)]
    for i in range(len(steps) + 1):
        if i < len(steps):
            j, q = steps[i]
            for start, size in CHUNKS:
                inner_rows(z_ref, g_ref, inv_ref, tc_ref, ts_ref, back.at[j % 2, q], j, q, start, size)
        if i > 0:
            last_rows(*steps[i - 1])

    for copy in copies:
        copy.wait()


def inverse(z, g, fac, inv, tc, ts, last):
    n = g.shape[0]
    return pl.pallas_call(
        functools.partial(inverse_kernel, n),
        in_specs=[pl.BlockSpec(memory_space=pltpu.VMEM)] * 7,
        out_specs=pl.BlockSpec(memory_space=pl.ANY),
        out_shape=jax.ShapeDtypeStruct((2 * HALF, RADIX, n, Q), jnp.float32),
        scratch_shapes=[
            pltpu.VMEM((2, 2, R, R), jnp.bfloat16),
            pltpu.VMEM((n, 2, HALF, R), jnp.float32),
            pltpu.SemaphoreType.DMA((n, 2 * RADIX)),
        ],
        compiler_params=pltpu.CompilerParams(vmem_limit_bytes=32 << 20),
        name="inverse",
    )(z, g, fac, inv, tc, ts, last)


def fill_slot(i, lanes):
    return slice(i * lanes, (i + 1) * lanes)


def forward(fr, fi, tc, ts, fwd_ref):
    tr = fr * tc + fi * ts
    ti = fi * tc - fr * ts
    r0, r1, r2, r3 = (tr[:, fill_slot(m, Q)] for m in range(RADIX))
    i0, i1, i2, i3 = (ti[:, fill_slot(m, Q)] for m in range(RADIX))
    ar, ai, br, bi = r0 + r2, i0 + i2, r0 - r2, i0 - i2
    cr, ci, dr, di = r1 + r3, i1 + i3, r1 - r3, i1 - i3
    parts = ((ar + cr, ai + ci), (br + di, bi - dr), (ar - cr, ai - ci), (br - di, bi + dr))
    return [
        dot(jnp.concatenate([half(x), half(y)], axis=1), fwd_ref[r])
        for r, (x, y) in enumerate(parts)
    ]


def torus(t, b):
    x, y_lo = lax.rem(b, 4), lax.div(b, 4)
    core, z, y_hi = lax.rem(t, 2), lax.rem(lax.div(t, 2), 4), lax.div(t, 8)
    y = 2 * y_hi + y_lo
    x_part = [lax.rem(x + d, 4) for d in range(4)]
    y_at = [lax.rem(y + d, 4) for d in range(4)]
    y_bank = [4 * lax.rem(v, 2) for v in y_at]
    y_tm = [8 * lax.div(v, 2) for v in y_at]
    z_part = [2 * lax.rem(z + d, 4) for d in range(4)]
    core_part = [core, 1 - core]

    def at(dx, dy, dz, dc):
        return {"tm": y_tm[dy] + z_part[dz] + core_part[dc], "bank": y_bank[dy] + x_part[dx]}

    def bank_at(dx, pair):
        other = lax.rem(y_lo + pair, 2)
        index = 4 * other + x_part[dx % 4]
        return index, {"tm": t, "bank": index}

    return at, bank_at


HOPS = (0, 1, 2, 1)
EVERYWHERE = sorted(
    [
        (dx, dy, dz, dc)
        for dx in range(4)
        for dy in range(4)
        for dz in range(4)
        for dc in range(2)
        if (dx, dy, dz, dc) != (0, 0, 0, 0)
    ],
    key=lambda d: -(HOPS[d[0]] + HOPS[d[1]] + HOPS[d[2]]),
)
ALONG_TM = [d for d in EVERYWHERE if d[0] == 0 and d[1] in (0, 2)]
BANK_PEERS = ((2, 1), (1, 1), (-1, 1), (2, 0), (1, 0), (-1, 0), (0, 1))


def spectrum_kernel(
    tm, bank, total_blocks,
    strain_ref, lens_hbm, tmpl_hbm, first_hbm, tc_hbm, ts_hbm, fwd_hbm,
    z_ref, g_ref, fac_ref,
    lens_ref, raw, blocks, prev, tmpl, first, tc, ts, fwd, zraw, send, recv, weights,
    load_sem, gather_send, gather_recv, sum_send, sum_recv, prev_send, prev_recv,
    share_send, share_recv,
):
    t = lax.axis_index("tm")
    b = lax.axis_index("bank")
    at, bank_at = torus(t, b)
    piece = HALF // bank
    band = HALF // bank
    tiles = band // 8 * RADIX

    barrier = pltpu.get_barrier_semaphore()
    for d in ALONG_TM:
        pl.semaphore_signal(barrier, 1, device_id=at(*d), device_id_type=MESH)
    for dx, pair in BANK_PEERS:
        pl.semaphore_signal(barrier, 1, device_id=bank_at(dx, pair)[1], device_id_type=MESH)

    loads = [(lens_hbm, lens_ref)]
    for c in range(2):
        for m in range(RADIX):
            loads.append((strain_ref.at[:, m, c, :], raw.at[c, :, pl.ds(m * Q, Q)]))
    loads += [(first_hbm, first), (tc_hbm, tc), (ts_hbm, ts), (fwd_hbm, fwd), (tmpl_hbm, tmpl)]
    loads = [pltpu.make_async_copy(s, d, load_sem.at[i]) for i, (s, d) in enumerate(loads)]
    for load in loads:
        load.start()

    for load in loads[: 2 * RADIX + 1]:
        load.wait()
    own_rows = pl.ds(pl.multiple_of(b * piece, piece), piece)
    position = (
        (lax.broadcasted_iota(jnp.int32, (piece, R), 0) + b * piece) * R
        + lax.broadcasted_iota(jnp.int32, (piece, R), 1)
    )
    for c in range(2):
        blocks[c, own_rows, :] = half(jnp.where(position < lens_ref[c], raw[c], 0.0))

    @pl.when(t == 0)
    def _():
        prev[...] = jnp.zeros_like(prev)

    pl.semaphore_wait(barrier, bank + tm - 2)

    def rows_of(index):
        return pl.ds(pl.multiple_of(index * piece, piece), piece)

    def gather(i, source, device):
        part = blocks.at[:, rows_of(source), :]
        return pltpu.make_async_remote_copy(
            src_ref=part,
            dst_ref=part,
            send_sem=gather_send.at[i],
            recv_sem=gather_recv.at[i],
            device_id=device,
            device_id_type=MESH,
        )

    outgoing = [gather(i, b, bank_at(dx, pair)[1]) for i, (dx, pair) in enumerate(BANK_PEERS)]
    incoming = [gather(i, *bank_at(-dx, pair)) for i, (dx, pair) in enumerate(BANK_PEERS)]
    for copy in outgoing:
        copy.start()

    for load in loads[2 * RADIX + 1 :]:
        load.wait()
    row = lax.broadcasted_iota(jnp.int32, (R, R), 0)
    col = lax.broadcasted_iota(jnp.int32, (R, R), 1)
    order = lax.rem(col, Q) * RADIX + lax.div(col, Q)
    pick = half(jnp.where(row == order, 1.0, 0.0))
    pick_mirror = half(jnp.where(row == R - 1 - order, 1.0, 0.0))
    up = lax.broadcasted_iota(jnp.int32, (ROWS, HALF), 0)
    across = lax.broadcasted_iota(jnp.int32, (ROWS, HALF), 1)
    flip = half(jnp.where(jnp.logical_and(across == HALF - up, across > 0), 1.0, 0.0))

    def join(j, carry):
        norm = jnp.zeros((1, R), jnp.float32)
        for p in range(2):
            direct = dot(tmpl[p, j, 0:ROWS, :], pick)
            mirror = dot(flip, half(dot(tmpl[p, j, HALF:R, :], pick_mirror)))
            joined = half(direct + mirror if p == 0 else direct - mirror)
            for r in range(RADIX):
                lo = (2 * r + p) * Q
                g_ref[j, :, lo : lo + Q] = joined[:, fill_slot(r, Q)]
            values = full(tmpl[p, j])
            norm = norm + jnp.sum(values * values, axis=0, keepdims=True)
        factor = lax.rsqrt(jnp.sum(norm, axis=1, keepdims=True))
        fac_ref[j] = jnp.broadcast_to(factor, (8, Q))
        return carry

    n = g_ref.shape[0]
    lax.fori_loop(0, n // 2, join, 0)

    for copy in incoming:
        copy.wait_recv()

    band_rows = pl.ds(pl.multiple_of(b * band, band), band)
    low_imag = pl.ds(pl.multiple_of(ROWS + b * band, 16), band)
    table = jnp.concatenate(
        [
            first[band_rows, 0:HALF],
            first[HALF:ROWS, 0:HALF],
            first[low_imag, 0:HALF],
            first[ROWS + HALF : 2 * ROWS, 0:HALF],
        ],
        axis=0,
    )
    band_tc = jnp.concatenate([tc[band_rows, :], tc[HALF:ROWS, :]], axis=0)
    band_ts = jnp.concatenate([ts[band_rows, :], ts[HALF:ROWS, :]], axis=0)
    power = [0.0] * RADIX
    height = band + ROWS - HALF
    for c in range(2):
        f = dot(table, blocks[c])
        spec = forward(f[:height], f[height:], band_tc, band_ts, fwd)
        for r in range(RADIX):
            re, im = spec[r][:, :Q], spec[r][:, Q:]
            power[r] = power[r] + (re * re + im * im)
    extra = jnp.concatenate(
        [power[r][band : band + 1] for r in range(RADIX)] + [jnp.zeros((8 - RADIX, Q), jnp.float32)],
        axis=0,
    )
    for i in range(tiles):
        low = i // RADIX * 8
        send[i] = half(jnp.concatenate([power[i % RADIX][low : low + 8], extra], axis=0))

    def sum_copy(i, device, slot):
        return pltpu.make_async_remote_copy(
            src_ref=send.at[slot],
            dst_ref=recv.at[i],
            send_sem=sum_send.at[i],
            recv_sem=sum_recv.at[i],
            device_id=device,
            device_id_type=MESH,
        )

    sums = []
    for i, d in enumerate(ALONG_TM):
        device = at(*d)
        sums.append(sum_copy(i, device, device["tm"]))
    for copy in sums:
        copy.start()

    next_copy = pltpu.make_async_remote_copy(
        src_ref=blocks.at[1],
        dst_ref=prev,
        send_sem=prev_send,
        recv_sem=prev_recv,
        device_id={"tm": lax.rem(t + 1, tm), "bank": b},
        device_id_type=MESH,
    )

    @pl.when(t < tm - 1)
    def _():
        next_copy.start()

    def region(q, now, before):
        f = dot(first[:, 0:HALF], now) + dot(first[:, HALF:R], before)
        spec = forward(f[:ROWS], f[ROWS:], tc[...], ts[...], fwd)
        for r in range(RADIX):
            zraw[q, :, fill_slot(r, 2 * Q)] = spec[r]

    region(1, blocks[1], blocks[0])

    total = full(send[t])
    for copy in sums:
        copy.wait_recv()
    for i in range(tm - 1):
        total = total + full(recv[i])
    weight = lax.rsqrt(total * (1.0 / total_blocks) + epsilon)
    me = b * tm + t
    weights[me] = half(weight[0:8])

    for d in EVERYWHERE:
        pltpu.make_async_remote_copy(
            src_ref=weights.at[me],
            dst_ref=weights.at[me],
            send_sem=share_send,
            recv_sem=share_recv,
            device_id=at(*d),
            device_id_type=MESH,
        ).start()

    lax.fori_loop(n // 2, n, join, 0)

    @pl.when(t > 0)
    def _():
        next_copy.wait_recv()

    region(0, blocks[0], prev[...])

    others = pltpu.make_async_remote_copy(
        src_ref=weights.at[pl.ds(0, tm * bank - 1)],
        dst_ref=weights.at[pl.ds(0, tm * bank - 1)],
        send_sem=share_send,
        recv_sem=share_recv,
        device_id={"tm": t, "bank": lax.rem(b + 1, bank)},
        device_id_type=MESH,
    )
    others.wait_recv()

    def whiten(i, carry):
        rows = pl.ds(pl.multiple_of(i * 16, 16), 16)
        for r in range(RADIX):
            tile = 2 * i * RADIX + r
            w = jnp.concatenate([full(weights[tile]), full(weights[tile + RADIX])], axis=0)
            for q in range(2):
                for p in range(2):
                    lanes = fill_slot(2 * r + p, Q)
                    z_ref[q, rows, lanes] = half(zraw[q, rows, lanes] * w)
        return carry

    lax.fori_loop(0, HALF // 16, whiten, 0)
    for r in range(RADIX):
        for q in range(2):
            for p in range(2):
                lanes = fill_slot(2 * r + p, Q)
                z_ref[q, HALF:ROWS, lanes] = half(
                    zraw[q, HALF:ROWS, lanes] * weight[8 + r : 9 + r]
                )

    for copy in outgoing:
        copy.wait_send()
    for copy in sums:
        copy.wait_send()

    @pl.when(t < tm - 1)
    def _():
        next_copy.wait_send()

    others.wait_send()


def spectra(strain, lengths, templates, tabs, tm, bank):
    n = templates.shape[1]
    first, tc, ts, fwd = tabs
    hbm = pl.BlockSpec(memory_space=pltpu.HBM)
    vmem = pl.BlockSpec(memory_space=pltpu.VMEM)
    bf, f32 = jnp.bfloat16, jnp.float32
    sem = pltpu.SemaphoreType.DMA
    pieces = strain.reshape(2, HALF // bank * RADIX, Q).transpose(1, 0, 2)
    pieces = pieces.reshape(HALF // bank, RADIX, 2, Q)
    return pl.pallas_call(
        functools.partial(spectrum_kernel, tm, bank, 2 * tm),
        in_specs=[hbm] * 7,
        out_specs=[vmem] * 3,
        out_shape=[
            jax.ShapeDtypeStruct((2, ROWS, 2 * R), bf),
            jax.ShapeDtypeStruct((n, ROWS, 2 * R), bf),
            jax.ShapeDtypeStruct((n, 8, Q), f32),
        ],
        scratch_shapes=[
            pltpu.SMEM((2,), jnp.int32),
            pltpu.VMEM((2, HALF // bank, R), f32),
            pltpu.VMEM((2, HALF, R), bf),
            pltpu.VMEM((HALF, R), bf),
            pltpu.VMEM((2, n, R, R), bf),
            pltpu.VMEM((2 * ROWS, R), bf),
            pltpu.VMEM((ROWS, R), f32),
            pltpu.VMEM((ROWS, R), f32),
            pltpu.VMEM((RADIX, HALF, HALF), bf),
            pltpu.VMEM((2, ROWS, 2 * R), f32),
            pltpu.VMEM((tm, 16, Q), bf),
            pltpu.VMEM((tm - 1, 16, Q), bf),
            pltpu.VMEM((tm * bank, 8, Q), bf),
            sem((2 * RADIX + 6,)),
            sem((bank - 1,)),
            sem((bank - 1,)),
            sem((tm,)),
            sem((tm,)),
            sem,
            sem,
            sem,
            sem,
        ],
        compiler_params=pltpu.CompilerParams(
            collective_id=0, has_side_effects=True, vmem_limit_bytes=32 << 20
        ),
        name="spectra",
    )(*[pltpu.with_memory_space_constraint(x, pltpu.HBM) for x in (pieces, lengths, templates, first, tc, ts, fwd)])


def body(tm, bank, strain, lengths, templates):
    first, tc, ts, fwd, inv, last = tables()
    bf = lambda x: jnp.asarray(x, jnp.bfloat16)
    f32 = lambda x: jnp.asarray(x, jnp.float32)
    tc, ts = f32(tc), f32(ts)
    z, g, fac = spectra(strain, lengths, templates, (bf(first), tc, ts, bf(fwd)), tm, bank)
    out = inverse(z, g, fac, bf(inv), tc, ts, bf(last))
    n = templates.shape[1]
    return out.reshape(2 * HALF * RADIX, n, Q).transpose(1, 0, 2).reshape(n, 2 * HALF * R)


def solution(mesh):
    in_specs = (P("tm", "bank"), P("tm"), P(None, "bank", None, None))
    step = functools.partial(body, mesh.shape["tm"], mesh.shape["bank"])
    return jax.shard_map(
        step, mesh=mesh, in_specs=in_specs, out_specs=P("bank", "tm"), check_vma=False
    )
```

```python
import functools
import math

import jax
import jax.numpy as jnp
import numpy as np
from jax import lax
from jax.experimental import pallas as pl
from jax.experimental.pallas import tpu as pltpu
from jax.sharding import PartitionSpec as P

R = 512
HALF = 256
ROWS = 272
RADIX = 4
Q = 128
epsilon = 1e-06
MESH = pl.DeviceIdType.MESH


def tables():
    k = np.arange(HALF + 1, dtype=np.int64)
    u = np.arange(R, dtype=np.int64)
    angle = 2.0 * math.pi * ((k[:, None] * u[None, :]) % R) / R
    first = np.zeros((2 * ROWS, R), np.float64)
    first[: HALF + 1] = np.cos(angle)
    first[ROWS : ROWS + HALF + 1] = -np.sin(angle)
    turn = 2.0 * math.pi * (k[:, None] * u[None, :]) / (R * R)
    tc = np.zeros((ROWS, R), np.float64)
    ts = np.zeros((ROWS, R), np.float64)
    tc[: HALF + 1] = np.cos(turn)
    ts[: HALF + 1] = np.sin(turn)
    v = np.arange(Q, dtype=np.int64)
    fwd = np.zeros((RADIX, HALF, HALF), np.float64)
    inv = np.zeros((RADIX, HALF, HALF), np.float64)
    for r in range(RADIX):
        phase = 2.0 * math.pi * ((v[:, None] * (RADIX * v[None, :] + r)) % R) / R
        c, s = np.cos(phase), np.sin(phase)
        fwd[r] = np.block([[c, -s], [s, c]])
        inv[r] = np.block([[c.T, s.T], [-s.T, c.T]])
    w = np.arange(HALF, dtype=np.int64)
    last = np.zeros((HALF, R), np.float64)
    phase = 2.0 * math.pi * ((w[:, None] * k[None, :HALF]) % R) / R
    last[:, :HALF] = np.cos(phase)
    last[:, HALF:] = -np.sin(phase)
    last[:, HALF] = 1.0 - 2.0 * (w % 2)
    return first, tc, ts, fwd, inv, last


def half(x):
    return x.astype(jnp.bfloat16)


def full(x):
    return x.astype(jnp.float32)


def dot(a, b):
    return jnp.dot(a, b, preferred_element_type=jnp.float32)


CHUNKS = ((0, 272),)


def inner_rows(z_ref, g_ref, inv_ref, tc_ref, ts_ref, back, j, q, start, size):
    rows = pl.ds(start, size)
    tr, ti = [], []
    for r in range(RADIX):
        lo = r * 2 * Q
        zr = z_ref[q, rows, lo : lo + Q]
        zi = z_ref[q, rows, lo + Q : lo + 2 * Q]
        gr = g_ref[j, rows, lo : lo + Q]
        gi = g_ref[j, rows, lo + Q : lo + 2 * Q]
        prod = jnp.concatenate([gr * zr + gi * zi, gr * zi - gi * zr], axis=1)
        t = dot(prod, inv_ref[r])
        tr.append(t[:, :Q])
        ti.append(t[:, Q:])
    ar, ai, br, bi = tr[0] + tr[2], ti[0] + ti[2], tr[0] - tr[2], ti[0] - ti[2]
    cr, ci, dr, di = tr[1] + tr[3], ti[1] + ti[3], tr[1] - tr[3], ti[1] - ti[3]
    inner = ((ar + cr, ai + ci), (br - di, bi + dr), (ar - cr, ai - ci), (br + di, bi - dr))
    for m in range(RADIX):
        lanes = slice(m * Q, (m + 1) * Q)
        ir, ii = half(inner[m][0]), half(inner[m][1])
        tc, ts = tc_ref[rows, lanes], ts_ref[rows, lanes]
        real = ir * tc - ii * ts
        imag = ii * tc + ir * ts
        keep = min(size, HALF - start)
        back[pl.ds(start, keep), lanes] = real[:keep]
        back[pl.ds(HALF + start, keep), lanes] = imag[:keep]
        if start + size == ROWS:
            top = back[HALF : HALF + 16, lanes]
            first_row = lax.broadcasted_iota(jnp.int32, (16, Q), 0) == 0
            back[HALF : HALF + 16, lanes] = half(
                jnp.where(first_row, full(real[keep : keep + 16]), full(top))
            )


def inverse_kernel(n, z_ref, g_ref, inv_ref, tc_ref, ts_ref, last_ref, out_ref, back, y, sem):
    copies = []

    def last_rows(j, q):
        y[j, q] = dot(last_ref[...], back[j % 2, q])
        for m in range(RADIX):
            copy = pltpu.make_async_copy(
                y.at[j, q, :, pl.ds(m * Q, Q)],
                out_ref.at[pl.ds(q * HALF, HALF), m, j, :],
                sem.at[j, q * RADIX + m],
            )
            copy.start()
            copies.append(copy)

    steps = [(j, q) for j in range(n) for q in range(2)]
    for i in range(len(steps) + 1):
        if i < len(steps):
            j, q = steps[i]
            for start, size in CHUNKS:
                inner_rows(z_ref, g_ref, inv_ref, tc_ref, ts_ref, back.at[j % 2, q], j, q, start, size)
        if i > 0:
            last_rows(*steps[i - 1])

    for copy in copies:
        copy.wait()


def inverse(z, g, inv, tc, ts, last):
    n = g.shape[0]
    return pl.pallas_call(
        functools.partial(inverse_kernel, n),
        in_specs=[pl.BlockSpec(memory_space=pltpu.VMEM)] * 6,
        out_specs=pl.BlockSpec(memory_space=pl.ANY),
        out_shape=jax.ShapeDtypeStruct((2 * HALF, RADIX, n, Q), jnp.float32),
        scratch_shapes=[
            pltpu.VMEM((2, 2, R, R), jnp.bfloat16),
            pltpu.VMEM((n, 2, HALF, R), jnp.float32),
            pltpu.SemaphoreType.DMA((n, 2 * RADIX)),
        ],
        compiler_params=pltpu.CompilerParams(vmem_limit_bytes=32 << 20),
        name="inverse",
    )(z, g, inv, tc, ts, last)


def fill_slot(i, lanes):
    return slice(i * lanes, (i + 1) * lanes)


def forward(fr, fi, tc, ts, fwd_ref):
    tr = fr * tc + fi * ts
    ti = fi * tc - fr * ts
    r0, r1, r2, r3 = (tr[:, fill_slot(m, Q)] for m in range(RADIX))
    i0, i1, i2, i3 = (ti[:, fill_slot(m, Q)] for m in range(RADIX))
    ar, ai, br, bi = r0 + r2, i0 + i2, r0 - r2, i0 - i2
    cr, ci, dr, di = r1 + r3, i1 + i3, r1 - r3, i1 - i3
    parts = ((ar + cr, ai + ci), (br + di, bi - dr), (ar - cr, ai - ci), (br - di, bi + dr))
    return [
        dot(jnp.concatenate([half(x), half(y)], axis=1), fwd_ref[r])
        for r, (x, y) in enumerate(parts)
    ]


def torus(t, b):
    x, y_lo = lax.rem(b, 4), lax.div(b, 4)
    core, z, y_hi = lax.rem(t, 2), lax.rem(lax.div(t, 2), 4), lax.div(t, 8)
    y = 2 * y_hi + y_lo
    x_part = [lax.rem(x + d, 4) for d in range(4)]
    y_at = [lax.rem(y + d, 4) for d in range(4)]
    y_bank = [4 * lax.rem(v, 2) for v in y_at]
    y_tm = [8 * lax.div(v, 2) for v in y_at]
    z_part = [2 * lax.rem(z + d, 4) for d in range(4)]
    core_part = [core, 1 - core]

    def at(dx, dy, dz, dc):
        return {"tm": y_tm[dy] + z_part[dz] + core_part[dc], "bank": y_bank[dy] + x_part[dx]}

    def bank_at(dx, pair):
        other = lax.rem(y_lo + pair, 2)
        index = 4 * other + x_part[dx % 4]
        return index, {"tm": t, "bank": index}

    def same_half(dx, pair, dz, dc):
        other = lax.rem(y_lo + pair, 2)
        return {"tm": 8 * y_hi + z_part[dz] + core_part[dc], "bank": 4 * other + x_part[dx]}

    return at, bank_at, same_half


HOPS = (0, 1, 2, 1)
EVERYWHERE = sorted(
    [
        (dx, dy, dz, dc)
        for dx in range(4)
        for dy in range(4)
        for dz in range(4)
        for dc in range(2)
        if (dx, dy, dz, dc) != (0, 0, 0, 0)
    ],
    key=lambda d: -(HOPS[d[0]] + HOPS[d[1]] + HOPS[d[2]]),
)
NEARER_HALF = sorted(
    [
        (dx, pair, dz, dc)
        for dx in range(4)
        for pair in range(2)
        for dz in range(4)
        for dc in range(2)
        if (dx, pair, dz, dc) != (0, 0, 0, 0)
    ],
    key=lambda d: -(HOPS[d[0]] + d[1] + HOPS[d[2]]),
)
ALONG_TM = [d for d in EVERYWHERE if d[0] == 0 and d[1] in (0, 2)]
BANK_PEERS = ((2, 1), (1, 1), (-1, 1), (2, 0), (1, 0), (-1, 0), (0, 1))


def spectrum_kernel(
    tm, bank, total_blocks,
    strain_ref, lens_hbm, tmpl_hbm, first_hbm, tc_hbm, ts_hbm, fwd_hbm,
    z_ref, g_ref, tc_ref, ts_ref,
    lens_ref, raw, blocks, prev, tmpl, first, tc, ts, fwd, zraw, send, recv, weights,
    load_sem, gather_send, gather_recv, sum_send, sum_recv, prev_send, prev_recv,
    share_send, share_recv,
):
    t = lax.axis_index("tm")
    b = lax.axis_index("bank")
    at, bank_at, same_half = torus(t, b)
    piece = HALF // bank
    band = HALF // bank
    tiles = band // 8 * RADIX
    owners = tm // 2
    per = tiles // owners
    own = lax.rem(t, owners)

    barrier = pltpu.get_barrier_semaphore()
    for d in ALONG_TM:
        pl.semaphore_signal(barrier, 1, device_id=at(*d), device_id_type=MESH)
    for dx, pair in BANK_PEERS:
        pl.semaphore_signal(barrier, 1, device_id=bank_at(dx, pair)[1], device_id_type=MESH)

    loads = [(lens_hbm, lens_ref)]
    for c in range(2):
        for m in range(RADIX):
            loads.append((strain_ref.at[:, m, c, :], raw.at[c, :, pl.ds(m * Q, Q)]))
    loads += [(first_hbm, first), (tc_hbm, tc), (ts_hbm, ts), (fwd_hbm, fwd), (tmpl_hbm, tmpl)]
    loads = [pltpu.make_async_copy(s, d, load_sem.at[i]) for i, (s, d) in enumerate(loads)]
    for load in loads:
        load.start()

    for load in loads[: 2 * RADIX + 1]:
        load.wait()
    own_rows = pl.ds(pl.multiple_of(b * piece, piece), piece)
    position = (
        (lax.broadcasted_iota(jnp.int32, (piece, R), 0) + b * piece) * R
        + lax.broadcasted_iota(jnp.int32, (piece, R), 1)
    )
    for c in range(2):
        blocks[c, own_rows, :] = half(jnp.where(position < lens_ref[c], raw[c], 0.0))

    @pl.when(t == 0)
    def _():
        prev[...] = jnp.zeros_like(prev)

    pl.semaphore_wait(barrier, bank + tm - 2)

    def rows_of(index):
        return pl.ds(pl.multiple_of(index * piece, piece), piece)

    def gather(i, source, device):
        part = blocks.at[:, rows_of(source), :]
        return pltpu.make_async_remote_copy(
            src_ref=part,
            dst_ref=part,
            send_sem=gather_send.at[i],
            recv_sem=gather_recv.at[i],
            device_id=device,
            device_id_type=MESH,
        )

    outgoing = [gather(i, b, bank_at(dx, pair)[1]) for i, (dx, pair) in enumerate(BANK_PEERS)]
    incoming = [gather(i, *bank_at(-dx, pair)) for i, (dx, pair) in enumerate(BANK_PEERS)]
    for copy in outgoing:
        copy.start()

    for load in loads[2 * RADIX + 1 :]:
        load.wait()
    tc_ref[...] = half(tc[...])
    ts_ref[...] = half(ts[...])
    row = lax.broadcasted_iota(jnp.int32, (R, R), 0)
    col = lax.broadcasted_iota(jnp.int32, (R, R), 1)
    order = lax.rem(col, Q) * RADIX + lax.div(col, Q)
    pick = half(jnp.where(row == order, 1.0, 0.0))
    pick_mirror = half(jnp.where(row == R - 1 - order, 1.0, 0.0))
    up = lax.broadcasted_iota(jnp.int32, (ROWS, HALF), 0)
    across = lax.broadcasted_iota(jnp.int32, (ROWS, HALF), 1)
    flip = half(jnp.where(jnp.logical_and(across == HALF - up, across > 0), 1.0, 0.0))

    def join(j, carry):
        norm = jnp.zeros((1, R), jnp.float32)
        for p in range(2):
            values = full(tmpl[p, j])
            norm = norm + jnp.sum(values * values, axis=0, keepdims=True)
        factor = lax.rsqrt(jnp.sum(norm, axis=1, keepdims=True))
        for p in range(2):
            direct = dot(tmpl[p, j, 0:ROWS, :], pick)
            mirror = dot(flip, half(dot(tmpl[p, j, HALF:R, :], pick_mirror)))
            joined = half((direct + mirror if p == 0 else direct - mirror) * factor)
            for r in range(RADIX):
                lo = (2 * r + p) * Q
                g_ref[j, :, lo : lo + Q] = joined[:, fill_slot(r, Q)]
        return carry

    n = g_ref.shape[0]
    lax.fori_loop(0, n // 2, join, 0)

    for copy in incoming:
        copy.wait_recv()

    band_rows = pl.ds(pl.multiple_of(b * band, band), band)
    low_imag = pl.ds(pl.multiple_of(ROWS + b * band, 16), band)
    table = jnp.concatenate(
        [
            first[band_rows, 0:HALF],
            first[HALF:ROWS, 0:HALF],
            first[low_imag, 0:HALF],
            first[ROWS + HALF : 2 * ROWS, 0:HALF],
        ],
        axis=0,
    )
    band_tc = jnp.concatenate([tc[band_rows, :], tc[HALF:ROWS, :]], axis=0)
    band_ts = jnp.concatenate([ts[band_rows, :], ts[HALF:ROWS, :]], axis=0)
    power = [0.0] * RADIX
    height = band + ROWS - HALF
    for c in range(2):
        f = dot(table, blocks[c])
        spec = forward(f[:height], f[height:], band_tc, band_ts, fwd)
        for r in range(RADIX):
            re, im = spec[r][:, :Q], spec[r][:, Q:]
            power[r] = power[r] + (re * re + im * im)
    extra = jnp.concatenate(
        [power[r][band : band + 1] for r in range(RADIX)] + [jnp.zeros((8 - RADIX, Q), jnp.float32)],
        axis=0,
    )
    for o in range(owners):
        parts = []
        for i in range(o * per, (o + 1) * per):
            low = i // RADIX * 8
            parts.append(power[i % RADIX][low : low + 8])
        parts += [extra, jnp.zeros((8, Q), jnp.float32)]
        send[o] = half(jnp.concatenate(parts, axis=0))

    def sum_copy(i, device, slot):
        return pltpu.make_async_remote_copy(
            src_ref=send.at[slot],
            dst_ref=recv.at[i],
            send_sem=sum_send.at[i],
            recv_sem=sum_recv.at[i],
            device_id=device,
            device_id_type=MESH,
        )

    sums = []
    for i, d in enumerate(ALONG_TM):
        device = at(*d)
        sums.append(sum_copy(i, device, lax.rem(device["tm"], owners)))
    for copy in sums:
        copy.start()

    next_copy = pltpu.make_async_remote_copy(
        src_ref=blocks.at[1],
        dst_ref=prev,
        send_sem=prev_send,
        recv_sem=prev_recv,
        device_id={"tm": lax.rem(t + 1, tm), "bank": b},
        device_id_type=MESH,
    )

    @pl.when(t < tm - 1)
    def _():
        next_copy.start()

    def region(q, now, before):
        f = dot(first[:, 0:HALF], now) + dot(first[:, HALF:R], before)
        spec = forward(f[:ROWS], f[ROWS:], tc[...], ts[...], fwd)
        for r in range(RADIX):
            zraw[q, :, fill_slot(r, 2 * Q)] = spec[r]

    region(1, blocks[1], blocks[0])

    total = full(send[own])
    for copy in sums:
        copy.wait_recv()
    for i in range(tm - 1):
        total = total + full(recv[i])
    weight = lax.rsqrt(total * (1.0 / total_blocks) + epsilon)
    mine = pl.ds(b * tiles + own * per, per)
    for i in range(per):
        weights[b * tiles + own * per + i] = half(weight[8 * i : 8 * i + 8])

    for d in NEARER_HALF:
        pltpu.make_async_remote_copy(
            src_ref=weights.at[mine],
            dst_ref=weights.at[mine],
            send_sem=share_send,
            recv_sem=share_recv,
            device_id=same_half(*d),
            device_id_type=MESH,
        ).start()

    lax.fori_loop(n // 2, n, join, 0)

    @pl.when(t > 0)
    def _():
        next_copy.wait_recv()

    region(0, blocks[0], prev[...])

    others = pltpu.make_async_remote_copy(
        src_ref=weights.at[pl.ds(0, tiles * bank - per)],
        dst_ref=weights.at[pl.ds(0, tiles * bank - per)],
        send_sem=share_send,
        recv_sem=share_recv,
        device_id={"tm": t, "bank": lax.rem(b + 1, bank)},
        device_id_type=MESH,
    )
    others.wait_recv()

    def whiten(i, carry):
        rows = pl.ds(pl.multiple_of(i * 16, 16), 16)
        for r in range(RADIX):
            tile = 2 * i * RADIX + r
            w = jnp.concatenate([full(weights[tile]), full(weights[tile + RADIX])], axis=0)
            for q in range(2):
                for p in range(2):
                    lanes = fill_slot(2 * r + p, Q)
                    z_ref[q, rows, lanes] = half(zraw[q, rows, lanes] * w)
        return carry

    lax.fori_loop(0, HALF // 16, whiten, 0)
    for r in range(RADIX):
        for q in range(2):
            for p in range(2):
                lanes = fill_slot(2 * r + p, Q)
                z_ref[q, HALF:ROWS, lanes] = half(
                    zraw[q, HALF:ROWS, lanes] * weight[8 * per + r : 8 * per + r + 1]
                )

    for copy in outgoing:
        copy.wait_send()
    for copy in sums:
        copy.wait_send()

    @pl.when(t < tm - 1)
    def _():
        next_copy.wait_send()

    others.wait_send()


def spectra(strain, lengths, templates, tabs, tm, bank):
    n = templates.shape[1]
    first, tc, ts, fwd = tabs
    hbm = pl.BlockSpec(memory_space=pltpu.HBM)
    vmem = pl.BlockSpec(memory_space=pltpu.VMEM)
    bf, f32 = jnp.bfloat16, jnp.float32
    sem = pltpu.SemaphoreType.DMA
    pieces = strain.reshape(2, HALF // bank * RADIX, Q).transpose(1, 0, 2)
    pieces = pieces.reshape(HALF // bank, RADIX, 2, Q)
    return pl.pallas_call(
        functools.partial(spectrum_kernel, tm, bank, 2 * tm),
        in_specs=[hbm] * 7,
        out_specs=[vmem] * 4,
        out_shape=[
            jax.ShapeDtypeStruct((2, ROWS, 2 * R), bf),
            jax.ShapeDtypeStruct((n, ROWS, 2 * R), bf),
            jax.ShapeDtypeStruct((ROWS, R), bf),
            jax.ShapeDtypeStruct((ROWS, R), bf),
        ],
        scratch_shapes=[
            pltpu.SMEM((2,), jnp.int32),
            pltpu.VMEM((2, HALF // bank, R), f32),
            pltpu.VMEM((2, HALF, R), bf),
            pltpu.VMEM((HALF, R), bf),
            pltpu.VMEM((2, n, R, R), bf),
            pltpu.VMEM((2 * ROWS, R), bf),
            pltpu.VMEM((ROWS, R), f32),
            pltpu.VMEM((ROWS, R), f32),
            pltpu.VMEM((RADIX, HALF, HALF), bf),
            pltpu.VMEM((2, ROWS, 2 * R), f32),
            pltpu.VMEM((tm // 2, 32, Q), bf),
            pltpu.VMEM((tm - 1, 32, Q), bf),
            pltpu.VMEM((HALF // 8 * RADIX, 8, Q), bf),
            sem((2 * RADIX + 6,)),
            sem((bank - 1,)),
            sem((bank - 1,)),
            sem((tm,)),
            sem((tm,)),
            sem,
            sem,
            sem,
            sem,
        ],
        compiler_params=pltpu.CompilerParams(
            collective_id=0, has_side_effects=True, vmem_limit_bytes=32 << 20
        ),
        name="spectra",
    )(*[pltpu.with_memory_space_constraint(x, pltpu.HBM) for x in (pieces, lengths, templates, first, tc, ts, fwd)])


def body(tm, bank, strain, lengths, templates):
    first, tc, ts, fwd, inv, last = tables()
    bf = lambda x: jnp.asarray(x, jnp.bfloat16)
    f32 = lambda x: jnp.asarray(x, jnp.float32)
    tc, ts = f32(tc), f32(ts)
    z, g, tc16, ts16 = spectra(strain, lengths, templates, (bf(first), tc, ts, bf(fwd)), tm, bank)
    out = inverse(z, g, bf(inv), tc16, ts16, bf(last))
    n = templates.shape[1]
    return out.reshape(2 * HALF * RADIX, n, Q).transpose(1, 0, 2).reshape(n, 2 * HALF * R)


def solution(mesh):
    in_specs = (P("tm", "bank"), P("tm"), P(None, "bank", None, None))
    step = functools.partial(body, mesh.shape["tm"], mesh.shape["bank"])
    return jax.shard_map(
        step, mesh=mesh, in_specs=in_specs, out_specs=P("bank", "tm"), check_vma=False
    )
```

```python
import functools
import math

import jax
import jax.numpy as jnp
import numpy as np
from jax import lax
from jax.experimental import pallas as pl
from jax.experimental.pallas import tpu as pltpu
from jax.sharding import PartitionSpec as P

R = 512
HALF = 256
ROWS = 272
RADIX = 4
Q = 128
epsilon = 1e-06
MESH = pl.DeviceIdType.MESH


def tables():
    k = np.arange(HALF + 1, dtype=np.int64)
    u = np.arange(R, dtype=np.int64)
    angle = 2.0 * math.pi * ((k[:, None] * u[None, :]) % R) / R
    first = np.zeros((2 * ROWS, R), np.float64)
    first[: HALF + 1] = np.cos(angle)
    first[ROWS : ROWS + HALF + 1] = -np.sin(angle)
    turn = 2.0 * math.pi * (k[:, None] * u[None, :]) / (R * R)
    tc = np.zeros((ROWS, R), np.float64)
    ts = np.zeros((ROWS, R), np.float64)
    tc[: HALF + 1] = np.cos(turn)
    ts[: HALF + 1] = np.sin(turn)
    v = np.arange(Q, dtype=np.int64)
    fwd = np.zeros((RADIX, HALF, HALF), np.float64)
    inv = np.zeros((RADIX, HALF, HALF), np.float64)
    for r in range(RADIX):
        phase = 2.0 * math.pi * ((v[:, None] * (RADIX * v[None, :] + r)) % R) / R
        c, s = np.cos(phase), np.sin(phase)
        fwd[r] = np.block([[c, -s], [s, c]])
        inv[r] = np.block([[c.T, s.T], [-s.T, c.T]])
    w = np.arange(HALF, dtype=np.int64)
    last = np.zeros((HALF, R), np.float64)
    phase = 2.0 * math.pi * ((w[:, None] * k[None, :HALF]) % R) / R
    last[:, :HALF] = np.cos(phase)
    last[:, HALF:] = -np.sin(phase)
    last[:, HALF] = 1.0 - 2.0 * (w % 2)
    return first, tc, ts, fwd, inv, last


def half(x):
    return x.astype(jnp.bfloat16)


def full(x):
    return x.astype(jnp.float32)


def dot(a, b):
    return jnp.dot(a, b, preferred_element_type=jnp.float32)


CHUNKS = ((0, 272),)


def inner_rows(z_ref, g_ref, inv_ref, tc_ref, ts_ref, back, j, q, start, size):
    rows = pl.ds(start, size)
    tr, ti = [], []
    for r in range(RADIX):
        lo = r * 2 * Q
        zr = z_ref[q, rows, lo : lo + Q]
        zi = z_ref[q, rows, lo + Q : lo + 2 * Q]
        gr = g_ref[j, rows, lo : lo + Q]
        gi = g_ref[j, rows, lo + Q : lo + 2 * Q]
        prod = jnp.concatenate([gr * zr + gi * zi, gr * zi - gi * zr], axis=1)
        t = dot(prod, inv_ref[r])
        tr.append(t[:, :Q])
        ti.append(t[:, Q:])
    ar, ai, br, bi = tr[0] + tr[2], ti[0] + ti[2], tr[0] - tr[2], ti[0] - ti[2]
    cr, ci, dr, di = tr[1] + tr[3], ti[1] + ti[3], tr[1] - tr[3], ti[1] - ti[3]
    inner = ((ar + cr, ai + ci), (br - di, bi + dr), (ar - cr, ai - ci), (br + di, bi - dr))
    for m in range(RADIX):
        lanes = slice(m * Q, (m + 1) * Q)
        ir, ii = half(inner[m][0]), half(inner[m][1])
        tc, ts = tc_ref[rows, lanes], ts_ref[rows, lanes]
        real = ir * tc - ii * ts
        imag = ii * tc + ir * ts
        keep = min(size, HALF - start)
        back[pl.ds(start, keep), lanes] = real[:keep]
        back[pl.ds(HALF + start, keep), lanes] = imag[:keep]
        if start + size == ROWS:
            top = back[HALF : HALF + 16, lanes]
            first_row = lax.broadcasted_iota(jnp.int32, (16, Q), 0) == 0
            back[HALF : HALF + 16, lanes] = half(
                jnp.where(first_row, full(real[keep : keep + 16]), full(top))
            )


def inverse_kernel(n, z_ref, g_ref, inv_ref, tc_ref, ts_ref, last_ref, out_ref, back, y, sem):
    copies = []

    def last_rows(j, q):
        y[j, q] = dot(last_ref[...], back[j % 2, q])
        for m in range(RADIX):
            copy = pltpu.make_async_copy(
                y.at[j, q, :, pl.ds(m * Q, Q)],
                out_ref.at[pl.ds(q * HALF, HALF), m, j, :],
                sem.at[j, q * RADIX + m],
            )
            copy.start()
            copies.append(copy)

    steps = [(j, q) for j in range(n) for q in range(2)]
    for i in range(len(steps) + 1):
        if i < len(steps):
            j, q = steps[i]
            for start, size in CHUNKS:
                inner_rows(z_ref, g_ref, inv_ref, tc_ref, ts_ref, back.at[j % 2, q], j, q, start, size)
        if i > 0:
            last_rows(*steps[i - 1])

    for copy in copies:
        copy.wait()


def inverse(z, g, inv, tc, ts, last):
    n = g.shape[0]
    return pl.pallas_call(
        functools.partial(inverse_kernel, n),
        in_specs=[pl.BlockSpec(memory_space=pltpu.VMEM)] * 6,
        out_specs=pl.BlockSpec(memory_space=pl.ANY),
        out_shape=jax.ShapeDtypeStruct((2 * HALF, RADIX, n, Q), jnp.float32),
        scratch_shapes=[
            pltpu.VMEM((2, 2, R, R), jnp.bfloat16),
            pltpu.VMEM((n, 2, HALF, R), jnp.float32),
            pltpu.SemaphoreType.DMA((n, 2 * RADIX)),
        ],
        compiler_params=pltpu.CompilerParams(vmem_limit_bytes=32 << 20),
        name="inverse",
    )(z, g, inv, tc, ts, last)


def fill_slot(i, lanes):
    return slice(i * lanes, (i + 1) * lanes)


def forward(fr, fi, tc, ts, fwd_ref):
    tr = fr * tc + fi * ts
    ti = fi * tc - fr * ts
    r0, r1, r2, r3 = (tr[:, fill_slot(m, Q)] for m in range(RADIX))
    i0, i1, i2, i3 = (ti[:, fill_slot(m, Q)] for m in range(RADIX))
    ar, ai, br, bi = r0 + r2, i0 + i2, r0 - r2, i0 - i2
    cr, ci, dr, di = r1 + r3, i1 + i3, r1 - r3, i1 - i3
    parts = ((ar + cr, ai + ci), (br + di, bi - dr), (ar - cr, ai - ci), (br - di, bi + dr))
    return [
        dot(jnp.concatenate([half(x), half(y)], axis=1), fwd_ref[r])
        for r, (x, y) in enumerate(parts)
    ]


def torus(t, b):
    x, y_lo = lax.rem(b, 4), lax.div(b, 4)
    core, z, y_hi = lax.rem(t, 2), lax.rem(lax.div(t, 2), 4), lax.div(t, 8)
    y = 2 * y_hi + y_lo
    x_part = [lax.rem(x + d, 4) for d in range(4)]
    y_at = [lax.rem(y + d, 4) for d in range(4)]
    y_bank = [4 * lax.rem(v, 2) for v in y_at]
    y_tm = [8 * lax.div(v, 2) for v in y_at]
    z_part = [2 * lax.rem(z + d, 4) for d in range(4)]
    core_part = [core, 1 - core]

    def at(dx, dy, dz, dc):
        return {"tm": y_tm[dy] + z_part[dz] + core_part[dc], "bank": y_bank[dy] + x_part[dx]}

    def bank_at(dx, pair):
        other = lax.rem(y_lo + pair, 2)
        index = 4 * other + x_part[dx % 4]
        return index, {"tm": t, "bank": index}

    def same_half(dx, pair, dz, dc):
        other = lax.rem(y_lo + pair, 2)
        return {"tm": 8 * y_hi + z_part[dz] + core_part[dc], "bank": 4 * other + x_part[dx]}

    return at, bank_at, same_half


HOPS = (0, 1, 2, 1)
EVERYWHERE = sorted(
    [
        (dx, dy, dz, dc)
        for dx in range(4)
        for dy in range(4)
        for dz in range(4)
        for dc in range(2)
        if (dx, dy, dz, dc) != (0, 0, 0, 0)
    ],
    key=lambda d: -(HOPS[d[0]] + HOPS[d[1]] + HOPS[d[2]]),
)
NEARER_HALF = sorted(
    [
        (dx, pair, dz, dc)
        for dx in range(4)
        for pair in range(2)
        for dz in range(4)
        for dc in range(2)
        if (dx, pair, dz, dc) != (0, 0, 0, 0)
    ],
    key=lambda d: -(HOPS[d[0]] + d[1] + HOPS[d[2]]),
)
NEXT_ALONG_TM = ((0, 0, 1, 0), (0, 0, 3, 0), (0, 2, 0, 0), (0, 0, 0, 1))
ALONG_TM = [d for d in EVERYWHERE if d[0] == 0 and d[1] in (0, 2)]
BANK_PEERS = ((2, 1), (1, 1), (-1, 1), (2, 0), (1, 0), (-1, 0), (0, 1))


def spectrum_kernel(
    tm, bank, total_blocks,
    strain_ref, lens_hbm, tmpl_hbm, first_hbm, tc_hbm, ts_hbm, fwd_hbm,
    z_ref, g_ref, tc_ref, ts_ref,
    lens_ref, raw, blocks, prev, tmpl, first, tc, ts, fwd, zraw, send, recv, weights,
    load_sem, gather_send, gather_recv, sum_send, sum_recv, prev_send, prev_recv,
    share_send, share_recv, word,
):
    t = lax.axis_index("tm")
    b = lax.axis_index("bank")
    at, bank_at, same_half = torus(t, b)
    piece = HALF // bank
    band = HALF // bank
    tiles = band // 8 * RADIX
    owners = tm // 2
    per = tiles // owners
    own = lax.rem(t, owners)

    loads = [(lens_hbm, lens_ref)]
    for c in range(2):
        for m in range(RADIX):
            loads.append((strain_ref.at[:, m, c, :], raw.at[c, :, pl.ds(m * Q, Q)]))
    loads += [(first_hbm, first), (tc_hbm, tc), (ts_hbm, ts), (fwd_hbm, fwd), (tmpl_hbm, tmpl)]
    loads = [pltpu.make_async_copy(s, d, load_sem.at[i]) for i, (s, d) in enumerate(loads)]
    for load in loads[: 2 * RADIX + 1]:
        load.start()

    barrier = pltpu.get_barrier_semaphore()
    for dx, pair in BANK_PEERS:
        pl.semaphore_signal(barrier, 1, device_id=bank_at(dx, pair)[1], device_id_type=MESH)
    for d in NEXT_ALONG_TM:
        pl.semaphore_signal(barrier, 1, device_id=at(*d), device_id_type=MESH)

    for load in loads[2 * RADIX + 1 :]:
        load.start()

    for load in loads[: 2 * RADIX + 1]:
        load.wait()
    own_rows = pl.ds(pl.multiple_of(b * piece, piece), piece)
    position = (
        (lax.broadcasted_iota(jnp.int32, (piece, R), 0) + b * piece) * R
        + lax.broadcasted_iota(jnp.int32, (piece, R), 1)
    )
    for c in range(2):
        blocks[c, own_rows, :] = half(jnp.where(position < lens_ref[c], raw[c], 0.0))

    @pl.when(t == 0)
    def _():
        prev[...] = jnp.zeros_like(prev)

    pl.semaphore_wait(barrier, bank - 1 + len(NEXT_ALONG_TM))

    def rows_of(index):
        return pl.ds(pl.multiple_of(index * piece, piece), piece)

    def gather(i, source, device):
        part = blocks.at[:, rows_of(source), :]
        return pltpu.make_async_remote_copy(
            src_ref=part,
            dst_ref=part,
            send_sem=gather_send.at[i],
            recv_sem=gather_recv.at[i],
            device_id=device,
            device_id_type=MESH,
        )

    outgoing = [gather(i, b, bank_at(dx, pair)[1]) for i, (dx, pair) in enumerate(BANK_PEERS)]
    incoming = [gather(i, *bank_at(-dx, pair)) for i, (dx, pair) in enumerate(BANK_PEERS)]
    for copy in outgoing:
        copy.start()

    def tell(i):
        for d in NEXT_ALONG_TM:
            pl.semaphore_signal(word.at[i], 1, device_id=at(*d), device_id_type=MESH)

    def hear(i):
        pl.semaphore_wait(word.at[i], len(NEXT_ALONG_TM))

    tell(0)

    for load in loads[2 * RADIX + 1 :]:
        load.wait()
    tc_ref[...] = half(tc[...])
    ts_ref[...] = half(ts[...])
    row = lax.broadcasted_iota(jnp.int32, (R, R), 0)
    col = lax.broadcasted_iota(jnp.int32, (R, R), 1)
    order = lax.rem(col, Q) * RADIX + lax.div(col, Q)
    pick = half(jnp.where(row == order, 1.0, 0.0))
    pick_mirror = half(jnp.where(row == R - 1 - order, 1.0, 0.0))
    up = lax.broadcasted_iota(jnp.int32, (ROWS, HALF), 0)
    across = lax.broadcasted_iota(jnp.int32, (ROWS, HALF), 1)
    flip = half(jnp.where(jnp.logical_and(across == HALF - up, across > 0), 1.0, 0.0))

    def join(j, carry):
        norm = jnp.zeros((1, R), jnp.float32)
        for p in range(2):
            values = full(tmpl[p, j])
            norm = norm + jnp.sum(values * values, axis=0, keepdims=True)
        factor = lax.rsqrt(jnp.sum(norm, axis=1, keepdims=True))
        for p in range(2):
            direct = dot(tmpl[p, j, 0:ROWS, :], pick)
            mirror = dot(flip, half(dot(tmpl[p, j, HALF:R, :], pick_mirror)))
            joined = half((direct + mirror if p == 0 else direct - mirror) * factor)
            for r in range(RADIX):
                lo = (2 * r + p) * Q
                g_ref[j, :, lo : lo + Q] = joined[:, fill_slot(r, Q)]
        return carry

    n = g_ref.shape[0]
    lax.fori_loop(0, 1, join, 0)
    hear(0)
    tell(1)
    lax.fori_loop(1, n // 2, join, 0)
    hear(1)
    tell(2)

    for copy in incoming:
        copy.wait_recv()

    band_rows = pl.ds(pl.multiple_of(b * band, band), band)
    low_imag = pl.ds(pl.multiple_of(ROWS + b * band, 16), band)
    table = jnp.concatenate(
        [
            first[band_rows, 0:HALF],
            first[HALF:ROWS, 0:HALF],
            first[low_imag, 0:HALF],
            first[ROWS + HALF : 2 * ROWS, 0:HALF],
        ],
        axis=0,
    )
    band_tc = jnp.concatenate([tc[band_rows, :], tc[HALF:ROWS, :]], axis=0)
    band_ts = jnp.concatenate([ts[band_rows, :], ts[HALF:ROWS, :]], axis=0)
    power = [0.0] * RADIX
    height = band + ROWS - HALF
    for c in range(2):
        f = dot(table, blocks[c])
        spec = forward(f[:height], f[height:], band_tc, band_ts, fwd)
        for r in range(RADIX):
            re, im = spec[r][:, :Q], spec[r][:, Q:]
            power[r] = power[r] + (re * re + im * im)
    extra = jnp.concatenate(
        [power[r][band : band + 1] for r in range(RADIX)] + [jnp.zeros((8 - RADIX, Q), jnp.float32)],
        axis=0,
    )
    for o in range(owners):
        parts = []
        for i in range(o * per, (o + 1) * per):
            low = i // RADIX * 8
            parts.append(power[i % RADIX][low : low + 8])
        parts += [extra, jnp.zeros((8, Q), jnp.float32)]
        send[o] = half(jnp.concatenate(parts, axis=0))

    def sum_copy(i, device, slot):
        return pltpu.make_async_remote_copy(
            src_ref=send.at[slot],
            dst_ref=recv.at[i],
            send_sem=sum_send.at[i],
            recv_sem=sum_recv.at[i],
            device_id=device,
            device_id_type=MESH,
        )

    sums = []
    for i, d in enumerate(ALONG_TM):
        device = at(*d)
        sums.append(sum_copy(i, device, lax.rem(device["tm"], owners)))
    hear(2)
    for copy in sums:
        copy.start()

    next_copy = pltpu.make_async_remote_copy(
        src_ref=blocks.at[1],
        dst_ref=prev,
        send_sem=prev_send,
        recv_sem=prev_recv,
        device_id={"tm": lax.rem(t + 1, tm), "bank": b},
        device_id_type=MESH,
    )

    @pl.when(t < tm - 1)
    def _():
        next_copy.start()

    def region(q, now, before):
        f = dot(first[:, 0:HALF], now) + dot(first[:, HALF:R], before)
        spec = forward(f[:ROWS], f[ROWS:], tc[...], ts[...], fwd)
        for r in range(RADIX):
            zraw[q, :, fill_slot(r, 2 * Q)] = spec[r]

    region(1, blocks[1], blocks[0])

    total = full(send[own])
    for copy in sums:
        copy.wait_recv()
    for i in range(tm - 1):
        total = total + full(recv[i])
    weight = lax.rsqrt(total * (1.0 / total_blocks) + epsilon)
    mine = pl.ds(b * tiles + own * per, per)
    for i in range(per):
        weights[b * tiles + own * per + i] = half(weight[8 * i : 8 * i + 8])

    for d in NEARER_HALF:
        pltpu.make_async_remote_copy(
            src_ref=weights.at[mine],
            dst_ref=weights.at[mine],
            send_sem=share_send,
            recv_sem=share_recv,
            device_id=same_half(*d),
            device_id_type=MESH,
        ).start()

    lax.fori_loop(n // 2, n, join, 0)

    @pl.when(t > 0)
    def _():
        next_copy.wait_recv()

    region(0, blocks[0], prev[...])

    others = pltpu.make_async_remote_copy(
        src_ref=weights.at[pl.ds(0, tiles * bank - per)],
        dst_ref=weights.at[pl.ds(0, tiles * bank - per)],
        send_sem=share_send,
        recv_sem=share_recv,
        device_id={"tm": t, "bank": lax.rem(b + 1, bank)},
        device_id_type=MESH,
    )
    others.wait_recv()

    def whiten(i, carry):
        rows = pl.ds(pl.multiple_of(i * 16, 16), 16)
        for r in range(RADIX):
            tile = 2 * i * RADIX + r
            w = jnp.concatenate([full(weights[tile]), full(weights[tile + RADIX])], axis=0)
            for q in range(2):
                for p in range(2):
                    lanes = fill_slot(2 * r + p, Q)
                    z_ref[q, rows, lanes] = half(zraw[q, rows, lanes] * w)
        return carry

    lax.fori_loop(0, HALF // 16, whiten, 0)
    for r in range(RADIX):
        for q in range(2):
            for p in range(2):
                lanes = fill_slot(2 * r + p, Q)
                z_ref[q, HALF:ROWS, lanes] = half(
                    zraw[q, HALF:ROWS, lanes] * weight[8 * per + r : 8 * per + r + 1]
                )

    for copy in outgoing:
        copy.wait_send()
    for copy in sums:
        copy.wait_send()

    @pl.when(t < tm - 1)
    def _():
        next_copy.wait_send()

    others.wait_send()


def spectra(strain, lengths, templates, tabs, tm, bank):
    n = templates.shape[1]
    first, tc, ts, fwd = tabs
    hbm = pl.BlockSpec(memory_space=pltpu.HBM)
    vmem = pl.BlockSpec(memory_space=pltpu.VMEM)
    bf, f32 = jnp.bfloat16, jnp.float32
    sem = pltpu.SemaphoreType.DMA
    pieces = strain.reshape(2, HALF // bank * RADIX, Q).transpose(1, 0, 2)
    pieces = pieces.reshape(HALF // bank, RADIX, 2, Q)
    return pl.pallas_call(
        functools.partial(spectrum_kernel, tm, bank, 2 * tm),
        in_specs=[hbm] * 7,
        out_specs=[vmem] * 4,
        out_shape=[
            jax.ShapeDtypeStruct((2, ROWS, 2 * R), bf),
            jax.ShapeDtypeStruct((n, ROWS, 2 * R), bf),
            jax.ShapeDtypeStruct((ROWS, R), bf),
            jax.ShapeDtypeStruct((ROWS, R), bf),
        ],
        scratch_shapes=[
            pltpu.SMEM((2,), jnp.int32),
            pltpu.VMEM((2, HALF // bank, R), f32),
            pltpu.VMEM((2, HALF, R), bf),
            pltpu.VMEM((HALF, R), bf),
            pltpu.VMEM((2, n, R, R), bf),
            pltpu.VMEM((2 * ROWS, R), bf),
            pltpu.VMEM((ROWS, R), f32),
            pltpu.VMEM((ROWS, R), f32),
            pltpu.VMEM((RADIX, HALF, HALF), bf),
            pltpu.VMEM((2, ROWS, 2 * R), f32),
            pltpu.VMEM((tm // 2, 32, Q), bf),
            pltpu.VMEM((tm - 1, 32, Q), bf),
            pltpu.VMEM((HALF // 8 * RADIX, 8, Q), bf),
            sem((2 * RADIX + 6,)),
            sem((bank - 1,)),
            sem((bank - 1,)),
            sem((tm,)),
            sem((tm,)),
            sem,
            sem,
            sem,
            sem,
            pltpu.SemaphoreType.REGULAR((3,)),
        ],
        compiler_params=pltpu.CompilerParams(
            collective_id=0, has_side_effects=True, vmem_limit_bytes=32 << 20
        ),
        name="spectra",
    )(*[pltpu.with_memory_space_constraint(x, pltpu.HBM) for x in (pieces, lengths, templates, first, tc, ts, fwd)])


def body(tm, bank, strain, lengths, templates):
    first, tc, ts, fwd, inv, last = tables()
    bf = lambda x: jnp.asarray(x, jnp.bfloat16)
    f32 = lambda x: jnp.asarray(x, jnp.float32)
    tc, ts = f32(tc), f32(ts)
    z, g, tc16, ts16 = spectra(strain, lengths, templates, (bf(first), tc, ts, bf(fwd)), tm, bank)
    out = inverse(z, g, bf(inv), tc16, ts16, bf(last))
    n = templates.shape[1]
    return out.reshape(2 * HALF * RADIX, n, Q).transpose(1, 0, 2).reshape(n, 2 * HALF * R)


def solution(mesh):
    in_specs = (P("tm", "bank"), P("tm"), P(None, "bank", None, None))
    step = functools.partial(body, mesh.shape["tm"], mesh.shape["bank"])
    return jax.shard_map(
        step, mesh=mesh, in_specs=in_specs, out_specs=P("bank", "tm"), check_vma=False
    )
```

```python
import functools
import math

import jax
import jax.numpy as jnp
import numpy as np
from jax import lax
from jax.experimental import pallas as pl
from jax.experimental.pallas import tpu as pltpu
from jax.sharding import PartitionSpec as P

R = 512
HALF = 256
ROWS = 272
RADIX = 4
Q = 128
epsilon = 1e-06
MESH = pl.DeviceIdType.MESH


def tables():
    k = np.arange(HALF + 1, dtype=np.int64)
    u = np.arange(R, dtype=np.int64)
    angle = 2.0 * math.pi * ((k[:, None] * u[None, :]) % R) / R
    first = np.zeros((2 * ROWS, R), np.float64)
    first[: HALF + 1] = np.cos(angle)
    first[ROWS : ROWS + HALF + 1] = -np.sin(angle)
    turn = 2.0 * math.pi * (k[:, None] * u[None, :]) / (R * R)
    tc = np.zeros((ROWS, R), np.float64)
    ts = np.zeros((ROWS, R), np.float64)
    tc[: HALF + 1] = np.cos(turn)
    ts[: HALF + 1] = np.sin(turn)
    v = np.arange(Q, dtype=np.int64)
    fwd = np.zeros((RADIX, HALF, HALF), np.float64)
    inv = np.zeros((RADIX, HALF, HALF), np.float64)
    for r in range(RADIX):
        phase = 2.0 * math.pi * ((v[:, None] * (RADIX * v[None, :] + r)) % R) / R
        c, s = np.cos(phase), np.sin(phase)
        fwd[r] = np.block([[c, -s], [s, c]])
        inv[r] = np.block([[c.T, s.T], [-s.T, c.T]])
    w = np.arange(HALF, dtype=np.int64)
    last = np.zeros((HALF, R), np.float64)
    phase = 2.0 * math.pi * ((w[:, None] * k[None, :HALF]) % R) / R
    last[:, :HALF] = np.cos(phase)
    last[:, HALF:] = -np.sin(phase)
    last[:, HALF] = 1.0 - 2.0 * (w % 2)
    return first, tc, ts, fwd, inv, last


def half(x):
    return x.astype(jnp.bfloat16)


def full(x):
    return x.astype(jnp.float32)


def dot(a, b):
    return jnp.dot(a, b, preferred_element_type=jnp.float32)


CHUNKS = ((0, 272),)


def inner_rows(z_ref, g_ref, inv_ref, tc_ref, ts_ref, back, j, q, start, size):
    rows = pl.ds(start, size)
    tr, ti = [], []
    for r in range(RADIX):
        lo = r * 2 * Q
        zr = z_ref[q, rows, lo : lo + Q]
        zi = z_ref[q, rows, lo + Q : lo + 2 * Q]
        gr = g_ref[j, rows, lo : lo + Q]
        gi = g_ref[j, rows, lo + Q : lo + 2 * Q]
        prod = jnp.concatenate([gr * zr + gi * zi, gr * zi - gi * zr], axis=1)
        t = dot(prod, inv_ref[r])
        tr.append(t[:, :Q])
        ti.append(t[:, Q:])
    ar, ai, br, bi = tr[0] + tr[2], ti[0] + ti[2], tr[0] - tr[2], ti[0] - ti[2]
    cr, ci, dr, di = tr[1] + tr[3], ti[1] + ti[3], tr[1] - tr[3], ti[1] - ti[3]
    inner = ((ar + cr, ai + ci), (br - di, bi + dr), (ar - cr, ai - ci), (br + di, bi - dr))
    for m in range(RADIX):
        lanes = slice(m * Q, (m + 1) * Q)
        ir, ii = half(inner[m][0]), half(inner[m][1])
        tc, ts = tc_ref[rows, lanes], ts_ref[rows, lanes]
        real = ir * tc - ii * ts
        imag = ii * tc + ir * ts
        keep = min(size, HALF - start)
        back[pl.ds(start, keep), lanes] = real[:keep]
        back[pl.ds(HALF + start, keep), lanes] = imag[:keep]
        if start + size == ROWS:
            top = back[HALF : HALF + 16, lanes]
            first_row = lax.broadcasted_iota(jnp.int32, (16, Q), 0) == 0
            back[HALF : HALF + 16, lanes] = half(
                jnp.where(first_row, full(real[keep : keep + 16]), full(top))
            )


def inverse_kernel(n, z_ref, g_ref, inv_ref, tc_ref, ts_ref, last_ref, out_ref, back, y, sem):
    copies = []

    def last_rows(j, q):
        y[j, pl.ds(q * HALF, HALF)] = dot(last_ref[...], back[j % 2, q])
        if q == 0 and j < n - 1:
            return
        at, size = (0, 2 * HALF) if j < n - 1 else (q * HALF, HALF)
        for m in range(RADIX):
            copy = pltpu.make_async_copy(
                y.at[j, pl.ds(at, size), pl.ds(m * Q, Q)],
                out_ref.at[pl.ds(at, size), m, j, :],
                sem.at[j, q * RADIX + m],
            )
            copy.start()
            copies.append(copy)

    steps = [(j, q) for j in range(n) for q in range(2)]
    for i in range(len(steps) + 1):
        if i < len(steps):
            j, q = steps[i]
            for start, size in CHUNKS:
                inner_rows(z_ref, g_ref, inv_ref, tc_ref, ts_ref, back.at[j % 2, q], j, q, start, size)
        if i > 0:
            last_rows(*steps[i - 1])

    for copy in copies:
        copy.wait()


def inverse(z, g, inv, tc, ts, last):
    n = g.shape[0]
    return pl.pallas_call(
        functools.partial(inverse_kernel, n),
        in_specs=[pl.BlockSpec(memory_space=pltpu.VMEM)] * 6,
        out_specs=pl.BlockSpec(memory_space=pl.ANY),
        out_shape=jax.ShapeDtypeStruct((2 * HALF, RADIX, n, Q), jnp.float32),
        scratch_shapes=[
            pltpu.VMEM((2, 2, R, R), jnp.bfloat16),
            pltpu.VMEM((n, 2 * HALF, R), jnp.float32),
            pltpu.SemaphoreType.DMA((n, 2 * RADIX)),
        ],
        compiler_params=pltpu.CompilerParams(vmem_limit_bytes=32 << 20),
        name="inverse",
    )(z, g, inv, tc, ts, last)


def fill_slot(i, lanes):
    return slice(i * lanes, (i + 1) * lanes)


def forward(fr, fi, tc, ts, fwd_ref):
    tr = fr * tc + fi * ts
    ti = fi * tc - fr * ts
    r0, r1, r2, r3 = (tr[:, fill_slot(m, Q)] for m in range(RADIX))
    i0, i1, i2, i3 = (ti[:, fill_slot(m, Q)] for m in range(RADIX))
    ar, ai, br, bi = r0 + r2, i0 + i2, r0 - r2, i0 - i2
    cr, ci, dr, di = r1 + r3, i1 + i3, r1 - r3, i1 - i3
    parts = ((ar + cr, ai + ci), (br + di, bi - dr), (ar - cr, ai - ci), (br - di, bi + dr))
    return [
        dot(jnp.concatenate([half(x), half(y)], axis=1), fwd_ref[r])
        for r, (x, y) in enumerate(parts)
    ]


def torus(t, b):
    x, y_lo = lax.rem(b, 4), lax.div(b, 4)
    core, z, y_hi = lax.rem(t, 2), lax.rem(lax.div(t, 2), 4), lax.div(t, 8)
    y = 2 * y_hi + y_lo
    x_part = [lax.rem(x + d, 4) for d in range(4)]
    y_at = [lax.rem(y + d, 4) for d in range(4)]
    y_bank = [4 * lax.rem(v, 2) for v in y_at]
    y_tm = [8 * lax.div(v, 2) for v in y_at]
    z_part = [2 * lax.rem(z + d, 4) for d in range(4)]
    core_part = [core, 1 - core]

    def at(dx, dy, dz, dc):
        return {"tm": y_tm[dy] + z_part[dz] + core_part[dc], "bank": y_bank[dy] + x_part[dx]}

    def bank_at(dx, pair):
        other = lax.rem(y_lo + pair, 2)
        index = 4 * other + x_part[dx % 4]
        return index, {"tm": t, "bank": index}

    def same_half(dx, pair, dz, dc):
        other = lax.rem(y_lo + pair, 2)
        return {"tm": 8 * y_hi + z_part[dz] + core_part[dc], "bank": 4 * other + x_part[dx]}

    return at, bank_at, same_half


HOPS = (0, 1, 2, 1)
EVERYWHERE = sorted(
    [
        (dx, dy, dz, dc)
        for dx in range(4)
        for dy in range(4)
        for dz in range(4)
        for dc in range(2)
        if (dx, dy, dz, dc) != (0, 0, 0, 0)
    ],
    key=lambda d: -(HOPS[d[0]] + HOPS[d[1]] + HOPS[d[2]]),
)
NEARER_HALF = sorted(
    [
        (dx, pair, dz, dc)
        for dx in range(4)
        for pair in range(2)
        for dz in range(4)
        for dc in range(2)
        if (dx, pair, dz, dc) != (0, 0, 0, 0)
    ],
    key=lambda d: -(HOPS[d[0]] + d[1] + HOPS[d[2]]),
)
NEXT_ALONG_TM = ((0, 0, 1, 0), (0, 0, 3, 0), (0, 2, 0, 0), (0, 0, 0, 1))
ALONG_TM = [d for d in EVERYWHERE if d[0] == 0 and d[1] in (0, 2)]
BANK_PEERS = ((2, 1), (1, 1), (-1, 1), (2, 0), (1, 0), (-1, 0), (0, 1))


def spectrum_kernel(
    tm, bank, total_blocks,
    strain_ref, lens_hbm, tmpl_hbm, first_hbm, tc_hbm, ts_hbm, fwd_hbm,
    z_ref, g_ref, tc_ref, ts_ref,
    lens_ref, raw, blocks, prev, tmpl, first, tc, ts, fwd, zraw, send, recv, weights,
    load_sem, gather_send, gather_recv, sum_send, sum_recv, prev_send, prev_recv,
    share_send, share_recv, word,
):
    t = lax.axis_index("tm")
    b = lax.axis_index("bank")
    at, bank_at, same_half = torus(t, b)
    piece = HALF // bank
    band = HALF // bank
    tiles = band // 8 * RADIX
    owners = tm // 2
    per = tiles // owners
    own = lax.rem(t, owners)

    loads = [(lens_hbm, lens_ref)]
    for c in range(2):
        for m in range(RADIX):
            loads.append((strain_ref.at[:, m, c, :], raw.at[c, :, pl.ds(m * Q, Q)]))
    loads += [(first_hbm, first), (tc_hbm, tc), (ts_hbm, ts), (fwd_hbm, fwd), (tmpl_hbm, tmpl)]
    loads = [pltpu.make_async_copy(s, d, load_sem.at[i]) for i, (s, d) in enumerate(loads)]
    for load in loads[: 2 * RADIX + 1]:
        load.start()

    barrier = pltpu.get_barrier_semaphore()
    for dx, pair in BANK_PEERS:
        pl.semaphore_signal(barrier, 1, device_id=bank_at(dx, pair)[1], device_id_type=MESH)
    for d in NEXT_ALONG_TM:
        pl.semaphore_signal(barrier, 1, device_id=at(*d), device_id_type=MESH)

    for load in loads[2 * RADIX + 1 :]:
        load.start()

    for load in loads[: 2 * RADIX + 1]:
        load.wait()
    own_rows = pl.ds(pl.multiple_of(b * piece, piece), piece)
    position = (
        (lax.broadcasted_iota(jnp.int32, (piece, R), 0) + b * piece) * R
        + lax.broadcasted_iota(jnp.int32, (piece, R), 1)
    )
    for c in range(2):
        blocks[c, own_rows, :] = half(jnp.where(position < lens_ref[c], raw[c], 0.0))

    @pl.when(t == 0)
    def _():
        prev[...] = jnp.zeros_like(prev)

    pl.semaphore_wait(barrier, bank - 1 + len(NEXT_ALONG_TM))

    def rows_of(index):
        return pl.ds(pl.multiple_of(index * piece, piece), piece)

    def gather(i, source, device):
        part = blocks.at[:, rows_of(source), :]
        return pltpu.make_async_remote_copy(
            src_ref=part,
            dst_ref=part,
            send_sem=gather_send.at[i],
            recv_sem=gather_recv.at[i],
            device_id=device,
            device_id_type=MESH,
        )

    outgoing = [gather(i, b, bank_at(dx, pair)[1]) for i, (dx, pair) in enumerate(BANK_PEERS)]
    incoming = [gather(i, *bank_at(-dx, pair)) for i, (dx, pair) in enumerate(BANK_PEERS)]
    for copy in outgoing:
        copy.start()

    def tell(i):
        for d in NEXT_ALONG_TM:
            pl.semaphore_signal(word.at[i], 1, device_id=at(*d), device_id_type=MESH)

    def hear(i):
        pl.semaphore_wait(word.at[i], len(NEXT_ALONG_TM))

    tell(0)

    for load in loads[2 * RADIX + 1 :]:
        load.wait()
    tc_ref[...] = half(tc[...])
    ts_ref[...] = half(ts[...])
    row = lax.broadcasted_iota(jnp.int32, (R, R), 0)
    col = lax.broadcasted_iota(jnp.int32, (R, R), 1)
    order = lax.rem(col, Q) * RADIX + lax.div(col, Q)
    pick = half(jnp.where(row == order, 1.0, 0.0))
    pick_mirror = half(jnp.where(row == R - 1 - order, 1.0, 0.0))
    up = lax.broadcasted_iota(jnp.int32, (ROWS, HALF), 0)
    across = lax.broadcasted_iota(jnp.int32, (ROWS, HALF), 1)
    flip = half(jnp.where(jnp.logical_and(across == HALF - up, across > 0), 1.0, 0.0))

    def join(j, carry):
        norm = jnp.zeros((1, R), jnp.float32)
        for p in range(2):
            values = full(tmpl[p, j])
            norm = norm + jnp.sum(values * values, axis=0, keepdims=True)
        factor = lax.rsqrt(jnp.sum(norm, axis=1, keepdims=True))
        for p in range(2):
            direct = dot(tmpl[p, j, 0:ROWS, :], pick)
            mirror = dot(flip, half(dot(tmpl[p, j, HALF:R, :], pick_mirror)))
            joined = half((direct + mirror if p == 0 else direct - mirror) * factor)
            for r in range(RADIX):
                lo = (2 * r + p) * Q
                g_ref[j, :, lo : lo + Q] = joined[:, fill_slot(r, Q)]
        return carry

    n = g_ref.shape[0]
    lax.fori_loop(0, 1, join, 0)
    hear(0)
    tell(1)
    lax.fori_loop(1, n // 2, join, 0)
    hear(1)
    tell(2)

    for copy in incoming:
        copy.wait_recv()

    band_rows = pl.ds(pl.multiple_of(b * band, band), band)
    low_imag = pl.ds(pl.multiple_of(ROWS + b * band, 16), band)
    table = jnp.concatenate(
        [
            first[band_rows, 0:HALF],
            first[HALF:ROWS, 0:HALF],
            first[low_imag, 0:HALF],
            first[ROWS + HALF : 2 * ROWS, 0:HALF],
        ],
        axis=0,
    )
    band_tc = jnp.concatenate([tc[band_rows, :], tc[HALF:ROWS, :]], axis=0)
    band_ts = jnp.concatenate([ts[band_rows, :], ts[HALF:ROWS, :]], axis=0)
    power = [0.0] * RADIX
    height = band + ROWS - HALF
    for c in range(2):
        f = dot(table, blocks[c])
        spec = forward(f[:height], f[height:], band_tc, band_ts, fwd)
        for r in range(RADIX):
            re, im = spec[r][:, :Q], spec[r][:, Q:]
            power[r] = power[r] + (re * re + im * im)
    extra = jnp.concatenate(
        [power[r][band : band + 1] for r in range(RADIX)] + [jnp.zeros((8 - RADIX, Q), jnp.float32)],
        axis=0,
    )
    for o in range(owners):
        parts = []
        for i in range(o * per, (o + 1) * per):
            low = i // RADIX * 8
            parts.append(power[i % RADIX][low : low + 8])
        parts += [extra, jnp.zeros((8, Q), jnp.float32)]
        send[o] = half(jnp.concatenate(parts, axis=0))

    def sum_copy(i, device, slot):
        return pltpu.make_async_remote_copy(
            src_ref=send.at[slot],
            dst_ref=recv.at[i],
            send_sem=sum_send.at[i],
            recv_sem=sum_recv.at[i],
            device_id=device,
            device_id_type=MESH,
        )

    sums = []
    for i, d in enumerate(ALONG_TM):
        device = at(*d)
        sums.append(sum_copy(i, device, lax.rem(device["tm"], owners)))
    hear(2)
    for copy in sums:
        copy.start()

    next_copy = pltpu.make_async_remote_copy(
        src_ref=blocks.at[1],
        dst_ref=prev,
        send_sem=prev_send,
        recv_sem=prev_recv,
        device_id={"tm": lax.rem(t + 1, tm), "bank": b},
        device_id_type=MESH,
    )

    @pl.when(t < tm - 1)
    def _():
        next_copy.start()

    def region(q, now, before):
        f = dot(first[:, 0:HALF], now) + dot(first[:, HALF:R], before)
        spec = forward(f[:ROWS], f[ROWS:], tc[...], ts[...], fwd)
        for r in range(RADIX):
            zraw[q, :, fill_slot(r, 2 * Q)] = spec[r]

    region(1, blocks[1], blocks[0])

    total = full(send[own])
    for copy in sums:
        copy.wait_recv()
    for i in range(tm - 1):
        total = total + full(recv[i])
    weight = lax.rsqrt(total * (1.0 / total_blocks) + epsilon)
    mine = pl.ds(b * tiles + own * per, per)
    for i in range(per):
        weights[b * tiles + own * per + i] = half(weight[8 * i : 8 * i + 8])

    for d in NEARER_HALF:
        pltpu.make_async_remote_copy(
            src_ref=weights.at[mine],
            dst_ref=weights.at[mine],
            send_sem=share_send,
            recv_sem=share_recv,
            device_id=same_half(*d),
            device_id_type=MESH,
        ).start()

    lax.fori_loop(n // 2, n, join, 0)

    @pl.when(t > 0)
    def _():
        next_copy.wait_recv()

    region(0, blocks[0], prev[...])

    others = pltpu.make_async_remote_copy(
        src_ref=weights.at[pl.ds(0, tiles * bank - per)],
        dst_ref=weights.at[pl.ds(0, tiles * bank - per)],
        send_sem=share_send,
        recv_sem=share_recv,
        device_id={"tm": t, "bank": lax.rem(b + 1, bank)},
        device_id_type=MESH,
    )
    others.wait_recv()

    def whiten(i, carry):
        rows = pl.ds(pl.multiple_of(i * 16, 16), 16)
        for r in range(RADIX):
            tile = 2 * i * RADIX + r
            w = jnp.concatenate([full(weights[tile]), full(weights[tile + RADIX])], axis=0)
            for q in range(2):
                for p in range(2):
                    lanes = fill_slot(2 * r + p, Q)
                    z_ref[q, rows, lanes] = half(zraw[q, rows, lanes] * w)
        return carry

    lax.fori_loop(0, HALF // 16, whiten, 0)
    for r in range(RADIX):
        for q in range(2):
            for p in range(2):
                lanes = fill_slot(2 * r + p, Q)
                z_ref[q, HALF:ROWS, lanes] = half(
                    zraw[q, HALF:ROWS, lanes] * weight[8 * per + r : 8 * per + r + 1]
                )

    for copy in outgoing:
        copy.wait_send()
    for copy in sums:
        copy.wait_send()

    @pl.when(t < tm - 1)
    def _():
        next_copy.wait_send()

    others.wait_send()


def spectra(strain, lengths, templates, tabs, tm, bank):
    n = templates.shape[1]
    first, tc, ts, fwd = tabs
    hbm = pl.BlockSpec(memory_space=pltpu.HBM)
    vmem = pl.BlockSpec(memory_space=pltpu.VMEM)
    bf, f32 = jnp.bfloat16, jnp.float32
    sem = pltpu.SemaphoreType.DMA
    pieces = strain.reshape(2, HALF // bank * RADIX, Q).transpose(1, 0, 2)
    pieces = pieces.reshape(HALF // bank, RADIX, 2, Q)
    return pl.pallas_call(
        functools.partial(spectrum_kernel, tm, bank, 2 * tm),
        in_specs=[hbm] * 7,
        out_specs=[vmem] * 4,
        out_shape=[
            jax.ShapeDtypeStruct((2, ROWS, 2 * R), bf),
            jax.ShapeDtypeStruct((n, ROWS, 2 * R), bf),
            jax.ShapeDtypeStruct((ROWS, R), bf),
            jax.ShapeDtypeStruct((ROWS, R), bf),
        ],
        scratch_shapes=[
            pltpu.SMEM((2,), jnp.int32),
            pltpu.VMEM((2, HALF // bank, R), f32),
            pltpu.VMEM((2, HALF, R), bf),
            pltpu.VMEM((HALF, R), bf),
            pltpu.VMEM((2, n, R, R), bf),
            pltpu.VMEM((2 * ROWS, R), bf),
            pltpu.VMEM((ROWS, R), f32),
            pltpu.VMEM((ROWS, R), f32),
            pltpu.VMEM((RADIX, HALF, HALF), bf),
            pltpu.VMEM((2, ROWS, 2 * R), f32),
            pltpu.VMEM((tm // 2, 32, Q), bf),
            pltpu.VMEM((tm - 1, 32, Q), bf),
            pltpu.VMEM((HALF // 8 * RADIX, 8, Q), bf),
            sem((2 * RADIX + 6,)),
            sem((bank - 1,)),
            sem((bank - 1,)),
            sem((tm,)),
            sem((tm,)),
            sem,
            sem,
            sem,
            sem,
            pltpu.SemaphoreType.REGULAR((3,)),
        ],
        compiler_params=pltpu.CompilerParams(
            collective_id=0, has_side_effects=True, vmem_limit_bytes=32 << 20
        ),
        name="spectra",
    )(*[pltpu.with_memory_space_constraint(x, pltpu.HBM) for x in (pieces, lengths, templates, first, tc, ts, fwd)])


def body(tm, bank, strain, lengths, templates):
    first, tc, ts, fwd, inv, last = tables()
    bf = lambda x: jnp.asarray(x, jnp.bfloat16)
    f32 = lambda x: jnp.asarray(x, jnp.float32)
    tc, ts = f32(tc), f32(ts)
    z, g, tc16, ts16 = spectra(strain, lengths, templates, (bf(first), tc, ts, bf(fwd)), tm, bank)
    out = inverse(z, g, bf(inv), tc16, ts16, bf(last))
    n = templates.shape[1]
    return out.reshape(2 * HALF * RADIX, n, Q).transpose(1, 0, 2).reshape(n, 2 * HALF * R)


def solution(mesh):
    in_specs = (P("tm", "bank"), P("tm"), P(None, "bank", None, None))
    step = functools.partial(body, mesh.shape["tm"], mesh.shape["bank"])
    return jax.shard_map(
        step, mesh=mesh, in_specs=in_specs, out_specs=P("bank", "tm"), check_vma=False
    )
```

```python
import functools
import math

import jax
import jax.numpy as jnp
import numpy as np
from jax import lax
from jax.experimental import pallas as pl
from jax.experimental.pallas import tpu as pltpu
from jax.sharding import PartitionSpec as P

R = 512
HALF = 256
ROWS = 272
RADIX = 4
Q = 128
epsilon = 1e-06
MESH = pl.DeviceIdType.MESH


def tables():
    k = np.arange(HALF + 1, dtype=np.int64)
    u = np.arange(R, dtype=np.int64)
    angle = 2.0 * math.pi * ((k[:, None] * u[None, :]) % R) / R
    first = np.zeros((2 * ROWS, R), np.float64)
    first[: HALF + 1] = np.cos(angle)
    first[ROWS : ROWS + HALF + 1] = -np.sin(angle)
    turn = 2.0 * math.pi * (k[:, None] * u[None, :]) / (R * R)
    tc = np.zeros((ROWS, R), np.float64)
    ts = np.zeros((ROWS, R), np.float64)
    tc[: HALF + 1] = np.cos(turn)
    ts[: HALF + 1] = np.sin(turn)
    v = np.arange(Q, dtype=np.int64)
    fwd = np.zeros((RADIX, HALF, HALF), np.float64)
    inv = np.zeros((RADIX, HALF, HALF), np.float64)
    for r in range(RADIX):
        phase = 2.0 * math.pi * ((v[:, None] * (RADIX * v[None, :] + r)) % R) / R
        c, s = np.cos(phase), np.sin(phase)
        fwd[r] = np.block([[c, -s], [s, c]])
        inv[r] = np.block([[c.T, s.T], [-s.T, c.T]])
    w = np.arange(HALF, dtype=np.int64)
    last = np.zeros((HALF, R), np.float64)
    phase = 2.0 * math.pi * ((w[:, None] * k[None, :HALF]) % R) / R
    last[:, :HALF] = np.cos(phase)
    last[:, HALF:] = -np.sin(phase)
    last[:, HALF] = 1.0 - 2.0 * (w % 2)
    return first, tc, ts, fwd, inv, last


def half(x):
    return x.astype(jnp.bfloat16)


def full(x):
    return x.astype(jnp.float32)


def dot(a, b):
    return jnp.dot(a, b, preferred_element_type=jnp.float32)


CHUNKS = ((0, 272),)


def inner_rows(z_ref, g_ref, inv_ref, tc_ref, ts_ref, back, j, q, start, size):
    rows = pl.ds(start, size)
    tr, ti = [], []
    for r in range(RADIX):
        lo = r * 2 * Q
        zr = z_ref[q, rows, lo : lo + Q]
        zi = z_ref[q, rows, lo + Q : lo + 2 * Q]
        gr = g_ref[j, rows, lo : lo + Q]
        gi = g_ref[j, rows, lo + Q : lo + 2 * Q]
        prod = jnp.concatenate([gr * zr + gi * zi, gr * zi - gi * zr], axis=1)
        t = dot(prod, inv_ref[r])
        tr.append(t[:, :Q])
        ti.append(t[:, Q:])
    ar, ai, br, bi = tr[0] + tr[2], ti[0] + ti[2], tr[0] - tr[2], ti[0] - ti[2]
    cr, ci, dr, di = tr[1] + tr[3], ti[1] + ti[3], tr[1] - tr[3], ti[1] - ti[3]
    inner = ((ar + cr, ai + ci), (br - di, bi + dr), (ar - cr, ai - ci), (br + di, bi - dr))
    for m in range(RADIX):
        lanes = slice(m * Q, (m + 1) * Q)
        ir, ii = half(inner[m][0]), half(inner[m][1])
        tc, ts = tc_ref[rows, lanes], ts_ref[rows, lanes]
        real = ir * tc - ii * ts
        imag = ii * tc + ir * ts
        keep = min(size, HALF - start)
        back[pl.ds(start, keep), lanes] = real[:keep]
        back[pl.ds(HALF + start, keep), lanes] = imag[:keep]
        if start + size == ROWS:
            top = back[HALF : HALF + 16, lanes]
            first_row = lax.broadcasted_iota(jnp.int32, (16, Q), 0) == 0
            back[HALF : HALF + 16, lanes] = half(
                jnp.where(first_row, full(real[keep : keep + 16]), full(top))
            )


def inverse_kernel(n, z_ref, g_ref, inv_ref, tc_ref, ts_ref, last_ref, out_ref, back, y, sem):
    copies = []

    def last_rows(j, q):
        y[j, pl.ds(q * HALF, HALF)] = dot(last_ref[...], back[j % 2, q])
        if q == 0 and j < n - 1:
            return
        at, size = (0, 2 * HALF) if j < n - 1 else (q * HALF, HALF)
        for m in range(RADIX):
            copy = pltpu.make_async_copy(
                y.at[j, pl.ds(at, size), pl.ds(m * Q, Q)],
                out_ref.at[pl.ds(at, size), m, j, :],
                sem.at[j, q * RADIX + m],
            )
            copy.start()
            copies.append(copy)

    steps = [(j, q) for j in range(n) for q in range(2)]
    for i in range(len(steps) + 1):
        if i < len(steps):
            j, q = steps[i]
            for start, size in CHUNKS:
                inner_rows(z_ref, g_ref, inv_ref, tc_ref, ts_ref, back.at[j % 2, q], j, q, start, size)
        if i > 0:
            last_rows(*steps[i - 1])

    for copy in copies:
        copy.wait()


def inverse(z, g, inv, tc, ts, last):
    n = g.shape[0]
    return pl.pallas_call(
        functools.partial(inverse_kernel, n),
        in_specs=[pl.BlockSpec(memory_space=pltpu.VMEM)] * 6,
        out_specs=pl.BlockSpec(memory_space=pl.ANY),
        out_shape=jax.ShapeDtypeStruct((2 * HALF, RADIX, n, Q), jnp.float32),
        scratch_shapes=[
            pltpu.VMEM((2, 2, R, R), jnp.bfloat16),
            pltpu.VMEM((n, 2 * HALF, R), jnp.float32),
            pltpu.SemaphoreType.DMA((n, 2 * RADIX)),
        ],
        compiler_params=pltpu.CompilerParams(vmem_limit_bytes=32 << 20),
        name="inverse",
    )(z, g, inv, tc, ts, last)


def fill_slot(i, lanes):
    return slice(i * lanes, (i + 1) * lanes)


def forward(fr, fi, tc, ts, fwd_ref):
    tr = fr * tc + fi * ts
    ti = fi * tc - fr * ts
    r0, r1, r2, r3 = (tr[:, fill_slot(m, Q)] for m in range(RADIX))
    i0, i1, i2, i3 = (ti[:, fill_slot(m, Q)] for m in range(RADIX))
    ar, ai, br, bi = r0 + r2, i0 + i2, r0 - r2, i0 - i2
    cr, ci, dr, di = r1 + r3, i1 + i3, r1 - r3, i1 - i3
    parts = ((ar + cr, ai + ci), (br + di, bi - dr), (ar - cr, ai - ci), (br - di, bi + dr))
    return [
        dot(jnp.concatenate([half(x), half(y)], axis=1), fwd_ref[r])
        for r, (x, y) in enumerate(parts)
    ]


def torus(t, b):
    x, y_lo = lax.rem(b, 4), lax.div(b, 4)
    core, z, y_hi = lax.rem(t, 2), lax.rem(lax.div(t, 2), 4), lax.div(t, 8)
    y = 2 * y_hi + y_lo
    x_part = [lax.rem(x + d, 4) for d in range(4)]
    y_at = [lax.rem(y + d, 4) for d in range(4)]
    y_bank = [4 * lax.rem(v, 2) for v in y_at]
    y_tm = [8 * lax.div(v, 2) for v in y_at]
    z_part = [2 * lax.rem(z + d, 4) for d in range(4)]
    core_part = [core, 1 - core]

    def at(dx, dy, dz, dc):
        return {"tm": y_tm[dy] + z_part[dz] + core_part[dc], "bank": y_bank[dy] + x_part[dx]}

    def bank_at(dx, pair):
        other = lax.rem(y_lo + pair, 2)
        index = 4 * other + x_part[dx % 4]
        return index, {"tm": t, "bank": index}

    def same_half(dx, pair, dz, dc):
        other = lax.rem(y_lo + pair, 2)
        return {"tm": 8 * y_hi + z_part[dz] + core_part[dc], "bank": 4 * other + x_part[dx]}

    return at, bank_at, same_half


HOPS = (0, 1, 2, 1)
EVERYWHERE = sorted(
    [
        (dx, dy, dz, dc)
        for dx in range(4)
        for dy in range(4)
        for dz in range(4)
        for dc in range(2)
        if (dx, dy, dz, dc) != (0, 0, 0, 0)
    ],
    key=lambda d: -(HOPS[d[0]] + HOPS[d[1]] + HOPS[d[2]]),
)
NEARER_HALF = sorted(
    [
        (dx, pair, dz, dc)
        for dx in range(4)
        for pair in range(2)
        for dz in range(4)
        for dc in range(2)
        if (dx, pair, dz, dc) != (0, 0, 0, 0)
    ],
    key=lambda d: -(HOPS[d[0]] + d[1] + HOPS[d[2]]),
)
NEXT_ALONG_TM = ((0, 0, 1, 0), (0, 0, 3, 0), (0, 2, 0, 0), (0, 0, 0, 1))
ALONG_TM = [d for d in EVERYWHERE if d[0] == 0 and d[1] in (0, 2)]
BANK_PEERS = ((2, 1), (1, 1), (-1, 1), (2, 0), (1, 0), (-1, 0), (0, 1))


def spectrum_kernel(
    tm, bank, total_blocks,
    strain_ref, lens_hbm, tmpl_hbm, first_hbm, tc_hbm, ts_hbm, fwd_hbm,
    z_ref, g_ref, tc_ref, ts_ref,
    lens_ref, raw, blocks, prev, tmpl, first, tc, ts, fwd, zraw, send, recv, weights,
    load_sem, gather_send, gather_recv, sum_send, sum_recv, prev_send, prev_recv,
    share_send, share_recv, word,
):
    loads = [(lens_hbm, lens_ref)]
    for c in range(2):
        for m in range(RADIX):
            loads.append((strain_ref.at[:, m, c, :], raw.at[c, :, pl.ds(m * Q, Q)]))
    loads += [(first_hbm, first), (tc_hbm, tc), (ts_hbm, ts), (fwd_hbm, fwd), (tmpl_hbm, tmpl)]
    loads = [pltpu.make_async_copy(s, d, load_sem.at[i]) for i, (s, d) in enumerate(loads)]
    for load in loads[: 2 * RADIX + 1]:
        load.start()

    t = lax.axis_index("tm")
    b = lax.axis_index("bank")
    at, bank_at, same_half = torus(t, b)
    piece = HALF // bank
    band = HALF // bank
    tiles = band // 8 * RADIX
    owners = tm // 2
    per = tiles // owners
    own = lax.rem(t, owners)

    barrier = pltpu.get_barrier_semaphore()
    for dx, pair in BANK_PEERS:
        pl.semaphore_signal(barrier, 1, device_id=bank_at(dx, pair)[1], device_id_type=MESH)
    for d in NEXT_ALONG_TM:
        pl.semaphore_signal(barrier, 1, device_id=at(*d), device_id_type=MESH)

    for load in loads[2 * RADIX + 1 :]:
        load.start()

    for load in loads[: 2 * RADIX + 1]:
        load.wait()
    own_rows = pl.ds(pl.multiple_of(b * piece, piece), piece)
    position = (
        (lax.broadcasted_iota(jnp.int32, (piece, R), 0) + b * piece) * R
        + lax.broadcasted_iota(jnp.int32, (piece, R), 1)
    )
    for c in range(2):
        blocks[c, own_rows, :] = half(jnp.where(position < lens_ref[c], raw[c], 0.0))

    @pl.when(t == 0)
    def _():
        prev[...] = jnp.zeros_like(prev)

    pl.semaphore_wait(barrier, bank - 1 + len(NEXT_ALONG_TM))

    def rows_of(index):
        return pl.ds(pl.multiple_of(index * piece, piece), piece)

    def gather(i, source, device):
        part = blocks.at[:, rows_of(source), :]
        return pltpu.make_async_remote_copy(
            src_ref=part,
            dst_ref=part,
            send_sem=gather_send.at[i],
            recv_sem=gather_recv.at[i],
            device_id=device,
            device_id_type=MESH,
        )

    outgoing = [gather(i, b, bank_at(dx, pair)[1]) for i, (dx, pair) in enumerate(BANK_PEERS)]
    incoming = [gather(i, *bank_at(-dx, pair)) for i, (dx, pair) in enumerate(BANK_PEERS)]
    for copy in outgoing:
        copy.start()

    def tell(i):
        for d in NEXT_ALONG_TM:
            pl.semaphore_signal(word.at[i], 1, device_id=at(*d), device_id_type=MESH)

    def hear(i):
        pl.semaphore_wait(word.at[i], len(NEXT_ALONG_TM))

    tell(0)

    for load in loads[2 * RADIX + 1 :]:
        load.wait()
    tc_ref[...] = half(tc[...])
    ts_ref[...] = half(ts[...])
    row = lax.broadcasted_iota(jnp.int32, (R, R), 0)
    col = lax.broadcasted_iota(jnp.int32, (R, R), 1)
    order = lax.rem(col, Q) * RADIX + lax.div(col, Q)
    pick = half(jnp.where(row == order, 1.0, 0.0))
    pick_mirror = half(jnp.where(row == R - 1 - order, 1.0, 0.0))
    up = lax.broadcasted_iota(jnp.int32, (ROWS, HALF), 0)
    across = lax.broadcasted_iota(jnp.int32, (ROWS, HALF), 1)
    flip = half(jnp.where(jnp.logical_and(across == HALF - up, across > 0), 1.0, 0.0))

    def join(j, carry):
        norm = jnp.zeros((1, R), jnp.float32)
        for p in range(2):
            values = full(tmpl[p, j])
            norm = norm + jnp.sum(values * values, axis=0, keepdims=True)
        factor = lax.rsqrt(jnp.sum(norm, axis=1, keepdims=True))
        for p in range(2):
            direct = dot(tmpl[p, j, 0:ROWS, :], pick)
            mirror = dot(flip, half(dot(tmpl[p, j, HALF:R, :], pick_mirror)))
            joined = half((direct + mirror if p == 0 else direct - mirror) * factor)
            for r in range(RADIX):
                lo = (2 * r + p) * Q
                g_ref[j, :, lo : lo + Q] = joined[:, fill_slot(r, Q)]
        return carry

    n = g_ref.shape[0]
    lax.fori_loop(0, 1, join, 0)
    hear(0)
    tell(1)
    lax.fori_loop(1, n // 2, join, 0)
    hear(1)
    tell(2)

    for copy in incoming:
        copy.wait_recv()

    band_rows = pl.ds(pl.multiple_of(b * band, band), band)
    low_imag = pl.ds(pl.multiple_of(ROWS + b * band, 16), band)
    table = jnp.concatenate(
        [
            first[band_rows, 0:HALF],
            first[HALF:ROWS, 0:HALF],
            first[low_imag, 0:HALF],
            first[ROWS + HALF : 2 * ROWS, 0:HALF],
        ],
        axis=0,
    )
    band_tc = jnp.concatenate([tc[band_rows, :], tc[HALF:ROWS, :]], axis=0)
    band_ts = jnp.concatenate([ts[band_rows, :], ts[HALF:ROWS, :]], axis=0)
    power = [0.0] * RADIX
    height = band + ROWS - HALF
    for c in range(2):
        f = dot(table, blocks[c])
        spec = forward(f[:height], f[height:], band_tc, band_ts, fwd)
        for r in range(RADIX):
            re, im = spec[r][:, :Q], spec[r][:, Q:]
            power[r] = power[r] + (re * re + im * im)
    extra = jnp.concatenate(
        [power[r][band : band + 1] for r in range(RADIX)] + [jnp.zeros((8 - RADIX, Q), jnp.float32)],
        axis=0,
    )
    for o in range(owners):
        for i in range(per):
            tile = o * per + i
            low = tile // RADIX * 8
            send[o, i] = half(power[tile % RADIX][low : low + 8])
        send[o, per] = half(extra)

    def sum_copy(i, device, slot):
        return pltpu.make_async_remote_copy(
            src_ref=send.at[slot],
            dst_ref=recv.at[i],
            send_sem=sum_send.at[i],
            recv_sem=sum_recv.at[i],
            device_id=device,
            device_id_type=MESH,
        )

    sums = []
    for i, d in enumerate(ALONG_TM):
        device = at(*d)
        sums.append(sum_copy(i, device, lax.rem(device["tm"], owners)))
    hear(2)
    for copy in sums:
        copy.start()

    next_copy = pltpu.make_async_remote_copy(
        src_ref=blocks.at[1],
        dst_ref=prev,
        send_sem=prev_send,
        recv_sem=prev_recv,
        device_id={"tm": lax.rem(t + 1, tm), "bank": b},
        device_id_type=MESH,
    )

    @pl.when(t < tm - 1)
    def _():
        next_copy.start()

    def region(q, now, before):
        f = dot(first[:, 0:HALF], now) + dot(first[:, HALF:R], before)
        spec = forward(f[:ROWS], f[ROWS:], tc[...], ts[...], fwd)
        for r in range(RADIX):
            zraw[q, :, fill_slot(r, 2 * Q)] = spec[r]

    region(1, blocks[1], blocks[0])

    total = [full(send[own, i]) for i in range(per + 1)]
    for copy in sums:
        copy.wait_recv()
    for k in range(tm - 1):
        total = [x + full(recv[k, i]) for i, x in enumerate(total)]
    weight = [lax.rsqrt(x * (1.0 / total_blocks) + epsilon) for x in total]
    mine = pl.ds(b * tiles + own * per, per)
    for i in range(per):
        weights[b * tiles + own * per + i] = half(weight[i])

    for d in NEARER_HALF:
        pltpu.make_async_remote_copy(
            src_ref=weights.at[mine],
            dst_ref=weights.at[mine],
            send_sem=share_send,
            recv_sem=share_recv,
            device_id=same_half(*d),
            device_id_type=MESH,
        ).start()

    lax.fori_loop(n // 2, n, join, 0)

    @pl.when(t > 0)
    def _():
        next_copy.wait_recv()

    region(0, blocks[0], prev[...])

    others = pltpu.make_async_remote_copy(
        src_ref=weights.at[pl.ds(0, tiles * bank - per)],
        dst_ref=weights.at[pl.ds(0, tiles * bank - per)],
        send_sem=share_send,
        recv_sem=share_recv,
        device_id={"tm": t, "bank": lax.rem(b + 1, bank)},
        device_id_type=MESH,
    )
    others.wait_recv()

    def whiten(i, carry):
        rows = pl.ds(pl.multiple_of(i * 16, 16), 16)
        for r in range(RADIX):
            tile = 2 * i * RADIX + r
            w = jnp.concatenate([full(weights[tile]), full(weights[tile + RADIX])], axis=0)
            for q in range(2):
                for p in range(2):
                    lanes = fill_slot(2 * r + p, Q)
                    z_ref[q, rows, lanes] = half(zraw[q, rows, lanes] * w)
        return carry

    lax.fori_loop(0, HALF // 16, whiten, 0)
    for r in range(RADIX):
        for q in range(2):
            for p in range(2):
                lanes = fill_slot(2 * r + p, Q)
                z_ref[q, HALF:ROWS, lanes] = half(
                    zraw[q, HALF:ROWS, lanes] * weight[per][r : r + 1]
                )

    for copy in outgoing:
        copy.wait_send()
    for copy in sums:
        copy.wait_send()

    @pl.when(t < tm - 1)
    def _():
        next_copy.wait_send()

    others.wait_send()


def spectra(strain, lengths, templates, tabs, tm, bank):
    n = templates.shape[1]
    first, tc, ts, fwd = tabs
    hbm = pl.BlockSpec(memory_space=pltpu.HBM)
    vmem = pl.BlockSpec(memory_space=pltpu.VMEM)
    bf, f32 = jnp.bfloat16, jnp.float32
    sem = pltpu.SemaphoreType.DMA
    pieces = strain.reshape(2, HALF // bank * RADIX, Q).transpose(1, 0, 2)
    pieces = pieces.reshape(HALF // bank, RADIX, 2, Q)
    return pl.pallas_call(
        functools.partial(spectrum_kernel, tm, bank, 2 * tm),
        in_specs=[hbm] * 7,
        out_specs=[vmem] * 4,
        out_shape=[
            jax.ShapeDtypeStruct((2, ROWS, 2 * R), bf),
            jax.ShapeDtypeStruct((n, ROWS, 2 * R), bf),
            jax.ShapeDtypeStruct((ROWS, R), bf),
            jax.ShapeDtypeStruct((ROWS, R), bf),
        ],
        scratch_shapes=[
            pltpu.SMEM((2,), jnp.int32),
            pltpu.VMEM((2, HALF // bank, R), f32),
            pltpu.VMEM((2, HALF, R), bf),
            pltpu.VMEM((HALF, R), bf),
            pltpu.VMEM((2, n, R, R), bf),
            pltpu.VMEM((2 * ROWS, R), bf),
            pltpu.VMEM((ROWS, R), f32),
            pltpu.VMEM((ROWS, R), f32),
            pltpu.VMEM((RADIX, HALF, HALF), bf),
            pltpu.VMEM((2, ROWS, 2 * R), f32),
            pltpu.VMEM((tm // 2, 3, 8, Q), bf),
            pltpu.VMEM((tm - 1, 3, 8, Q), bf),
            pltpu.VMEM((HALF // 8 * RADIX, 8, Q), bf),
            sem((2 * RADIX + 6,)),
            sem((bank - 1,)),
            sem((bank - 1,)),
            sem((tm,)),
            sem((tm,)),
            sem,
            sem,
            sem,
            sem,
            pltpu.SemaphoreType.REGULAR((3,)),
        ],
        compiler_params=pltpu.CompilerParams(
            collective_id=0, has_side_effects=True, vmem_limit_bytes=32 << 20
        ),
        name="spectra",
    )(*[pltpu.with_memory_space_constraint(x, pltpu.HBM) for x in (pieces, lengths, templates, first, tc, ts, fwd)])


def body(tm, bank, strain, lengths, templates):
    first, tc, ts, fwd, inv, last = tables()
    bf = lambda x: jnp.asarray(x, jnp.bfloat16)
    f32 = lambda x: jnp.asarray(x, jnp.float32)
    tc, ts = f32(tc), f32(ts)
    z, g, tc16, ts16 = spectra(strain, lengths, templates, (bf(first), tc, ts, bf(fwd)), tm, bank)
    out = inverse(z, g, bf(inv), tc16, ts16, bf(last))
    n = templates.shape[1]
    return out.reshape(2 * HALF * RADIX, n, Q).transpose(1, 0, 2).reshape(n, 2 * HALF * R)


def solution(mesh):
    in_specs = (P("tm", "bank"), P("tm"), P(None, "bank", None, None))
    step = functools.partial(body, mesh.shape["tm"], mesh.shape["bank"])
    return jax.shard_map(
        step, mesh=mesh, in_specs=in_specs, out_specs=P("bank", "tm"), check_vma=False
    )
```

```python
import functools
import math

import jax
import jax.numpy as jnp
import numpy as np
from jax import lax
from jax.experimental import pallas as pl
from jax.experimental.pallas import tpu as pltpu
from jax.sharding import PartitionSpec as P

R = 512
HALF = 256
ROWS = 272
RADIX = 4
Q = 128
epsilon = 1e-06
MESH = pl.DeviceIdType.MESH


def tables():
    k = np.arange(HALF + 1, dtype=np.int64)
    u = np.arange(R, dtype=np.int64)
    angle = 2.0 * math.pi * ((k[:, None] * u[None, :]) % R) / R
    first = np.zeros((2 * ROWS, R), np.float64)
    first[: HALF + 1] = np.cos(angle)
    first[ROWS : ROWS + HALF + 1] = -np.sin(angle)
    turn = 2.0 * math.pi * (k[:, None] * u[None, :]) / (R * R)
    tc = np.zeros((ROWS, R), np.float64)
    ts = np.zeros((ROWS, R), np.float64)
    tc[: HALF + 1] = np.cos(turn)
    ts[: HALF + 1] = np.sin(turn)
    v = np.arange(Q, dtype=np.int64)
    fwd = np.zeros((RADIX, HALF, HALF), np.float64)
    inv = np.zeros((RADIX, HALF, HALF), np.float64)
    for r in range(RADIX):
        phase = 2.0 * math.pi * ((v[:, None] * (RADIX * v[None, :] + r)) % R) / R
        c, s = np.cos(phase), np.sin(phase)
        fwd[r] = np.block([[c, -s], [s, c]])
        inv[r] = np.block([[c.T, s.T], [-s.T, c.T]])
    w = np.arange(HALF, dtype=np.int64)
    last = np.zeros((HALF, R), np.float64)
    phase = 2.0 * math.pi * ((w[:, None] * k[None, :HALF]) % R) / R
    last[:, :HALF] = np.cos(phase)
    last[:, HALF:] = -np.sin(phase)
    last[:, HALF] = 1.0 - 2.0 * (w % 2)
    return first, tc, ts, fwd, inv, last


def half(x):
    return x.astype(jnp.bfloat16)


def full(x):
    return x.astype(jnp.float32)


def dot(a, b):
    return jnp.dot(a, b, preferred_element_type=jnp.float32)


CHUNKS = ((0, 272),)


def inner_rows(z_ref, g_ref, inv_ref, tc_ref, ts_ref, back, j, q, start, size):
    rows = pl.ds(start, size)
    tr, ti = [], []
    for r in range(RADIX):
        lo = r * 2 * Q
        zr = z_ref[q, rows, lo : lo + Q]
        zi = z_ref[q, rows, lo + Q : lo + 2 * Q]
        gr = g_ref[j, rows, lo : lo + Q]
        gi = g_ref[j, rows, lo + Q : lo + 2 * Q]
        prod = jnp.concatenate([gr * zr + gi * zi, gr * zi - gi * zr], axis=1)
        t = dot(prod, inv_ref[r])
        tr.append(t[:, :Q])
        ti.append(t[:, Q:])
    ar, ai, br, bi = tr[0] + tr[2], ti[0] + ti[2], tr[0] - tr[2], ti[0] - ti[2]
    cr, ci, dr, di = tr[1] + tr[3], ti[1] + ti[3], tr[1] - tr[3], ti[1] - ti[3]
    inner = ((ar + cr, ai + ci), (br - di, bi + dr), (ar - cr, ai - ci), (br + di, bi - dr))
    for m in range(RADIX):
        lanes = slice(m * Q, (m + 1) * Q)
        ir, ii = half(inner[m][0]), half(inner[m][1])
        tc, ts = tc_ref[rows, lanes], ts_ref[rows, lanes]
        real = ir * tc - ii * ts
        imag = ii * tc + ir * ts
        keep = min(size, HALF - start)
        back[pl.ds(start, keep), lanes] = real[:keep]
        back[pl.ds(HALF + start, keep), lanes] = imag[:keep]
        if start + size == ROWS:
            top = back[HALF : HALF + 16, lanes]
            first_row = lax.broadcasted_iota(jnp.int32, (16, Q), 0) == 0
            back[HALF : HALF + 16, lanes] = half(
                jnp.where(first_row, full(real[keep : keep + 16]), full(top))
            )


def inverse_kernel(n, z_ref, g_ref, inv_ref, tc_ref, ts_ref, last_ref, out_ref, back, y, sem):
    copies = []

    def last_rows(j, q):
        final = j == n - 1
        at, size = (q * HALF, HALF) if final else (0, 2 * HALF)
        for m in range(RADIX):
            if m % 2 == 0:
                lanes = pl.ds(m * Q, 2 * Q)
                y[j, pl.ds(q * HALF, HALF), lanes] = dot(last_ref[...], back[j % 2, q, :, lanes])
            if q == 0 and not final:
                continue
            copy = pltpu.make_async_copy(
                y.at[j, pl.ds(at, size), pl.ds(m * Q, Q)],
                out_ref.at[pl.ds(at, size), m, j, :],
                sem.at[j, q * RADIX + m],
            )
            copy.start()
            copies.append(copy)

    steps = [(j, q) for j in range(n) for q in range(2)]
    for i in range(len(steps) + 1):
        if i < len(steps):
            j, q = steps[i]
            for start, size in CHUNKS:
                inner_rows(z_ref, g_ref, inv_ref, tc_ref, ts_ref, back.at[j % 2, q], j, q, start, size)
        if i > 0:
            last_rows(*steps[i - 1])

    for copy in copies:
        copy.wait()


def inverse(z, g, inv, tc, ts, last):
    n = g.shape[0]
    return pl.pallas_call(
        functools.partial(inverse_kernel, n),
        in_specs=[pl.BlockSpec(memory_space=pltpu.VMEM)] * 6,
        out_specs=pl.BlockSpec(memory_space=pl.ANY),
        out_shape=jax.ShapeDtypeStruct((2 * HALF, RADIX, n, Q), jnp.float32),
        scratch_shapes=[
            pltpu.VMEM((2, 2, R, R), jnp.bfloat16),
            pltpu.VMEM((n, 2 * HALF, R), jnp.float32),
            pltpu.SemaphoreType.DMA((n, 2 * RADIX)),
        ],
        compiler_params=pltpu.CompilerParams(vmem_limit_bytes=32 << 20),
        name="inverse",
    )(z, g, inv, tc, ts, last)


def fill_slot(i, lanes):
    return slice(i * lanes, (i + 1) * lanes)


def forward(fr, fi, tc, ts, fwd_ref):
    tr = fr * tc + fi * ts
    ti = fi * tc - fr * ts
    r0, r1, r2, r3 = (tr[:, fill_slot(m, Q)] for m in range(RADIX))
    i0, i1, i2, i3 = (ti[:, fill_slot(m, Q)] for m in range(RADIX))
    ar, ai, br, bi = r0 + r2, i0 + i2, r0 - r2, i0 - i2
    cr, ci, dr, di = r1 + r3, i1 + i3, r1 - r3, i1 - i3
    parts = ((ar + cr, ai + ci), (br + di, bi - dr), (ar - cr, ai - ci), (br - di, bi + dr))
    return [
        dot(jnp.concatenate([half(x), half(y)], axis=1), fwd_ref[r])
        for r, (x, y) in enumerate(parts)
    ]


def torus(t, b):
    x, y_lo = lax.rem(b, 4), lax.div(b, 4)
    core, z, y_hi = lax.rem(t, 2), lax.rem(lax.div(t, 2), 4), lax.div(t, 8)
    y = 2 * y_hi + y_lo
    x_part = [lax.rem(x + d, 4) for d in range(4)]
    y_at = [lax.rem(y + d, 4) for d in range(4)]
    y_bank = [4 * lax.rem(v, 2) for v in y_at]
    y_tm = [8 * lax.div(v, 2) for v in y_at]
    z_part = [2 * lax.rem(z + d, 4) for d in range(4)]
    core_part = [core, 1 - core]

    def at(dx, dy, dz, dc):
        return {"tm": y_tm[dy] + z_part[dz] + core_part[dc], "bank": y_bank[dy] + x_part[dx]}

    def bank_at(dx, pair):
        other = lax.rem(y_lo + pair, 2)
        index = 4 * other + x_part[dx % 4]
        return index, {"tm": t, "bank": index}

    def same_half(dx, pair, dz, dc):
        other = lax.rem(y_lo + pair, 2)
        return {"tm": 8 * y_hi + z_part[dz] + core_part[dc], "bank": 4 * other + x_part[dx]}

    return at, bank_at, same_half


HOPS = (0, 1, 2, 1)
EVERYWHERE = sorted(
    [
        (dx, dy, dz, dc)
        for dx in range(4)
        for dy in range(4)
        for dz in range(4)
        for dc in range(2)
        if (dx, dy, dz, dc) != (0, 0, 0, 0)
    ],
    key=lambda d: -(HOPS[d[0]] + HOPS[d[1]] + HOPS[d[2]]),
)
NEARER_HALF = sorted(
    [
        (dx, pair, dz, dc)
        for dx in range(4)
        for pair in range(2)
        for dz in range(4)
        for dc in range(2)
        if (dx, pair, dz, dc) != (0, 0, 0, 0)
    ],
    key=lambda d: -(HOPS[d[0]] + d[1] + HOPS[d[2]]),
)
NEXT_ALONG_TM = ((0, 0, 1, 0), (0, 0, 3, 0), (0, 2, 0, 0), (0, 0, 0, 1))
ALONG_TM = [d for d in EVERYWHERE if d[0] == 0 and d[1] in (0, 2)]
BANK_PEERS = ((2, 1), (1, 1), (-1, 1), (2, 0), (1, 0), (-1, 0), (0, 1))


def spectrum_kernel(
    tm, bank, total_blocks,
    strain_ref, lens_hbm, tmpl_hbm, first_hbm, tc_hbm, ts_hbm, fwd_hbm,
    z_ref, g_ref, tc_ref, ts_ref,
    lens_ref, raw, blocks, prev, tmpl, first, tc, ts, fwd, zraw, send, recv, weights,
    load_sem, gather_send, gather_recv, sum_send, sum_recv, prev_send, prev_recv,
    share_send, share_recv, word,
):
    loads = [(lens_hbm, lens_ref)]
    for c in range(2):
        for m in range(RADIX):
            loads.append((strain_ref.at[:, m, c, :], raw.at[c, :, pl.ds(m * Q, Q)]))
    loads += [(first_hbm, first), (tc_hbm, tc), (ts_hbm, ts), (fwd_hbm, fwd), (tmpl_hbm, tmpl)]
    loads = [pltpu.make_async_copy(s, d, load_sem.at[i]) for i, (s, d) in enumerate(loads)]
    for load in loads[: 2 * RADIX + 1]:
        load.start()

    t = lax.axis_index("tm")
    b = lax.axis_index("bank")
    at, bank_at, same_half = torus(t, b)
    piece = HALF // bank
    band = HALF // bank
    tiles = band // 8 * RADIX
    owners = tm // 2
    per = tiles // owners
    own = lax.rem(t, owners)

    barrier = pltpu.get_barrier_semaphore()
    for dx, pair in BANK_PEERS:
        pl.semaphore_signal(barrier, 1, device_id=bank_at(dx, pair)[1], device_id_type=MESH)
    for d in NEXT_ALONG_TM:
        pl.semaphore_signal(barrier, 1, device_id=at(*d), device_id_type=MESH)

    for load in loads[2 * RADIX + 1 :]:
        load.start()

    for load in loads[: 2 * RADIX + 1]:
        load.wait()
    own_rows = pl.ds(pl.multiple_of(b * piece, piece), piece)
    position = (
        (lax.broadcasted_iota(jnp.int32, (piece, R), 0) + b * piece) * R
        + lax.broadcasted_iota(jnp.int32, (piece, R), 1)
    )
    for c in range(2):
        blocks[c, own_rows, :] = half(jnp.where(position < lens_ref[c], raw[c], 0.0))

    @pl.when(t == 0)
    def _():
        prev[...] = jnp.zeros_like(prev)

    pl.semaphore_wait(barrier, bank - 1 + len(NEXT_ALONG_TM))

    def rows_of(index):
        return pl.ds(pl.multiple_of(index * piece, piece), piece)

    def gather(i, source, device):
        part = blocks.at[:, rows_of(source), :]
        return pltpu.make_async_remote_copy(
            src_ref=part,
            dst_ref=part,
            send_sem=gather_send.at[i],
            recv_sem=gather_recv.at[i],
            device_id=device,
            device_id_type=MESH,
        )

    outgoing = [gather(i, b, bank_at(dx, pair)[1]) for i, (dx, pair) in enumerate(BANK_PEERS)]
    incoming = [gather(i, *bank_at(-dx, pair)) for i, (dx, pair) in enumerate(BANK_PEERS)]
    for copy in outgoing:
        copy.start()

    def tell(i):
        for d in NEXT_ALONG_TM:
            pl.semaphore_signal(word.at[i], 1, device_id=at(*d), device_id_type=MESH)

    def hear(i):
        pl.semaphore_wait(word.at[i], len(NEXT_ALONG_TM))

    tell(0)

    for load in loads[2 * RADIX + 1 :]:
        load.wait()
    tc_ref[...] = half(tc[...])
    ts_ref[...] = half(ts[...])
    row = lax.broadcasted_iota(jnp.int32, (R, R), 0)
    col = lax.broadcasted_iota(jnp.int32, (R, R), 1)
    order = lax.rem(col, Q) * RADIX + lax.div(col, Q)
    pick = half(jnp.where(row == order, 1.0, 0.0))
    pick_mirror = half(jnp.where(row == R - 1 - order, 1.0, 0.0))
    up = lax.broadcasted_iota(jnp.int32, (ROWS, HALF), 0)
    across = lax.broadcasted_iota(jnp.int32, (ROWS, HALF), 1)
    flip = half(jnp.where(jnp.logical_and(across == HALF - up, across > 0), 1.0, 0.0))

    def join(j, carry):
        norm = jnp.zeros((1, R), jnp.float32)
        for p in range(2):
            values = full(tmpl[p, j])
            norm = norm + jnp.sum(values * values, axis=0, keepdims=True)
        factor = lax.rsqrt(jnp.sum(norm, axis=1, keepdims=True))
        for p in range(2):
            direct = dot(tmpl[p, j, 0:ROWS, :], pick)
            mirror = dot(flip, half(dot(tmpl[p, j, HALF:R, :], pick_mirror)))
            joined = half((direct + mirror if p == 0 else direct - mirror) * factor)
            for r in range(RADIX):
                lo = (2 * r + p) * Q
                g_ref[j, :, lo : lo + Q] = joined[:, fill_slot(r, Q)]
        return carry

    n = g_ref.shape[0]
    lax.fori_loop(0, 1, join, 0)
    hear(0)
    tell(1)
    lax.fori_loop(1, n // 2, join, 0)
    hear(1)
    tell(2)

    for copy in incoming:
        copy.wait_recv()

    band_rows = pl.ds(pl.multiple_of(b * band, band), band)
    low_imag = pl.ds(pl.multiple_of(ROWS + b * band, 16), band)
    table = jnp.concatenate(
        [
            first[band_rows, 0:HALF],
            first[HALF:ROWS, 0:HALF],
            first[low_imag, 0:HALF],
            first[ROWS + HALF : 2 * ROWS, 0:HALF],
        ],
        axis=0,
    )
    band_tc = jnp.concatenate([tc[band_rows, :], tc[HALF:ROWS, :]], axis=0)
    band_ts = jnp.concatenate([ts[band_rows, :], ts[HALF:ROWS, :]], axis=0)
    power = [0.0] * RADIX
    height = band + ROWS - HALF
    for c in range(2):
        f = dot(table, blocks[c])
        spec = forward(f[:height], f[height:], band_tc, band_ts, fwd)
        for r in range(RADIX):
            re, im = spec[r][:, :Q], spec[r][:, Q:]
            power[r] = power[r] + (re * re + im * im)
    extra = jnp.concatenate(
        [power[r][band : band + 1] for r in range(RADIX)] + [jnp.zeros((8 - RADIX, Q), jnp.float32)],
        axis=0,
    )
    for o in range(owners):
        for i in range(per):
            tile = o * per + i
            low = tile // RADIX * 8
            send[o, i] = half(power[tile % RADIX][low : low + 8])
        send[o, per] = half(extra)

    def sum_copy(i, device, slot):
        return pltpu.make_async_remote_copy(
            src_ref=send.at[slot],
            dst_ref=recv.at[i],
            send_sem=sum_send.at[i],
            recv_sem=sum_recv.at[i],
            device_id=device,
            device_id_type=MESH,
        )

    sums = []
    for i, d in enumerate(ALONG_TM):
        device = at(*d)
        sums.append(sum_copy(i, device, lax.rem(device["tm"], owners)))
    hear(2)
    for copy in sums:
        copy.start()

    next_copy = pltpu.make_async_remote_copy(
        src_ref=blocks.at[1],
        dst_ref=prev,
        send_sem=prev_send,
        recv_sem=prev_recv,
        device_id={"tm": lax.rem(t + 1, tm), "bank": b},
        device_id_type=MESH,
    )

    @pl.when(t < tm - 1)
    def _():
        next_copy.start()

    def region(q, now, before):
        f = dot(first[:, 0:HALF], now) + dot(first[:, HALF:R], before)
        spec = forward(f[:ROWS], f[ROWS:], tc[...], ts[...], fwd)
        for r in range(RADIX):
            zraw[q, :, fill_slot(r, 2 * Q)] = spec[r]

    region(1, blocks[1], blocks[0])

    total = [full(send[own, i]) for i in range(per + 1)]
    for copy in sums:
        copy.wait_recv()
    for k in range(tm - 1):
        total = [x + full(recv[k, i]) for i, x in enumerate(total)]
    weight = [lax.rsqrt(x * (1.0 / total_blocks) + epsilon) for x in total]
    mine = pl.ds(b * tiles + own * per, per)
    for i in range(per):
        weights[b * tiles + own * per + i] = half(weight[i])

    for d in NEARER_HALF:
        pltpu.make_async_remote_copy(
            src_ref=weights.at[mine],
            dst_ref=weights.at[mine],
            send_sem=share_send,
            recv_sem=share_recv,
            device_id=same_half(*d),
            device_id_type=MESH,
        ).start()

    lax.fori_loop(n // 2, n, join, 0)

    @pl.when(t > 0)
    def _():
        next_copy.wait_recv()

    region(0, blocks[0], prev[...])

    others = pltpu.make_async_remote_copy(
        src_ref=weights.at[pl.ds(0, tiles * bank - per)],
        dst_ref=weights.at[pl.ds(0, tiles * bank - per)],
        send_sem=share_send,
        recv_sem=share_recv,
        device_id={"tm": t, "bank": lax.rem(b + 1, bank)},
        device_id_type=MESH,
    )
    others.wait_recv()

    def whiten(i, carry):
        rows = pl.ds(pl.multiple_of(i * 16, 16), 16)
        for r in range(RADIX):
            tile = 2 * i * RADIX + r
            w = jnp.concatenate([full(weights[tile]), full(weights[tile + RADIX])], axis=0)
            for q in range(2):
                for p in range(2):
                    lanes = fill_slot(2 * r + p, Q)
                    z_ref[q, rows, lanes] = half(zraw[q, rows, lanes] * w)
        return carry

    lax.fori_loop(0, HALF // 16, whiten, 0)
    for r in range(RADIX):
        for q in range(2):
            for p in range(2):
                lanes = fill_slot(2 * r + p, Q)
                z_ref[q, HALF:ROWS, lanes] = half(
                    zraw[q, HALF:ROWS, lanes] * weight[per][r : r + 1]
                )

    for copy in outgoing:
        copy.wait_send()
    for copy in sums:
        copy.wait_send()

    @pl.when(t < tm - 1)
    def _():
        next_copy.wait_send()

    others.wait_send()


def spectra(strain, lengths, templates, tabs, tm, bank):
    n = templates.shape[1]
    first, tc, ts, fwd = tabs
    hbm = pl.BlockSpec(memory_space=pltpu.HBM)
    vmem = pl.BlockSpec(memory_space=pltpu.VMEM)
    bf, f32 = jnp.bfloat16, jnp.float32
    sem = pltpu.SemaphoreType.DMA
    pieces = strain.reshape(2, HALF // bank * RADIX, Q).transpose(1, 0, 2)
    pieces = pieces.reshape(HALF // bank, RADIX, 2, Q)
    return pl.pallas_call(
        functools.partial(spectrum_kernel, tm, bank, 2 * tm),
        in_specs=[hbm] * 7,
        out_specs=[vmem] * 4,
        out_shape=[
            jax.ShapeDtypeStruct((2, ROWS, 2 * R), bf),
            jax.ShapeDtypeStruct((n, ROWS, 2 * R), bf),
            jax.ShapeDtypeStruct((ROWS, R), bf),
            jax.ShapeDtypeStruct((ROWS, R), bf),
        ],
        scratch_shapes=[
            pltpu.SMEM((2,), jnp.int32),
            pltpu.VMEM((2, HALF // bank, R), f32),
            pltpu.VMEM((2, HALF, R), bf),
            pltpu.VMEM((HALF, R), bf),
            pltpu.VMEM((2, n, R, R), bf),
            pltpu.VMEM((2 * ROWS, R), bf),
            pltpu.VMEM((ROWS, R), f32),
            pltpu.VMEM((ROWS, R), f32),
            pltpu.VMEM((RADIX, HALF, HALF), bf),
            pltpu.VMEM((2, ROWS, 2 * R), f32),
            pltpu.VMEM((tm // 2, 3, 8, Q), bf),
            pltpu.VMEM((tm - 1, 3, 8, Q), bf),
            pltpu.VMEM((HALF // 8 * RADIX, 8, Q), bf),
            sem((2 * RADIX + 6,)),
            sem((bank - 1,)),
            sem((bank - 1,)),
            sem((tm,)),
            sem((tm,)),
            sem,
            sem,
            sem,
            sem,
            pltpu.SemaphoreType.REGULAR((3,)),
        ],
        compiler_params=pltpu.CompilerParams(
            collective_id=0, has_side_effects=True, vmem_limit_bytes=32 << 20
        ),
        name="spectra",
    )(*[pltpu.with_memory_space_constraint(x, pltpu.HBM) for x in (pieces, lengths, templates, first, tc, ts, fwd)])


def body(tm, bank, strain, lengths, templates):
    first, tc, ts, fwd, inv, last = tables()
    bf = lambda x: jnp.asarray(x, jnp.bfloat16)
    f32 = lambda x: jnp.asarray(x, jnp.float32)
    tc, ts = f32(tc), f32(ts)
    z, g, tc16, ts16 = spectra(strain, lengths, templates, (bf(first), tc, ts, bf(fwd)), tm, bank)
    out = inverse(z, g, bf(inv), tc16, ts16, bf(last))
    n = templates.shape[1]
    return out.reshape(2 * HALF * RADIX, n, Q).transpose(1, 0, 2).reshape(n, 2 * HALF * R)


def solution(mesh):
    in_specs = (P("tm", "bank"), P("tm"), P(None, "bank", None, None))
    step = functools.partial(body, mesh.shape["tm"], mesh.shape["bank"])
    return jax.shard_map(
        step, mesh=mesh, in_specs=in_specs, out_specs=P("bank", "tm"), check_vma=False
    )
```
